256 devices in a mesh: row: 16 (over x_lo, y, core), col: 16 (over z, x_hi).
Axes of the slice: x: 4 (x_hi: 2, x_lo: 2; x = x_hi * 2 + x_lo), y: 4, z: 8, core: 2. Of those that a mesh axis runs over, the one named last changes fastest.
Arguments:
- matrix: float32 [12288, 12288], P('row', 'col'), as said below
- left_panel: float32 [12288, 1024], P('row', 'col'), may hold values from -2.5 to 2.5
- right_panel: float32 [12288, 1024], P('row', 'col'), may hold values from -2.5 to 2.5
- reflectors: float32 [12288, 256], P('row', 'col'), may hold values from -0.109375 to 0.109375
Outputs:
- updated: float32 [12288, 12288], P('row', 'col')
The draws below stay inside these ranges and needn't reach their ends.
Inputs may be any that keep to these rules, and one draw needn't show every extreme that they name: matrix is exactly skew-symmetric.
All inputs are finite; a program needn't handle non-finite values.
Results may differ from the reference program's by a relative error of at most 0.00011.
Values sent between devices are 32-bit elements; how exact they have to be, the bound alone decides.
A program may use at most 128 MiB of HBM per device.

```python
import jax
import jax.numpy as jnp
from jax import lax

NB = 256
N = 12288
K = 1024


def draw_matrix(key, part):
    normal_part = jax.random.normal(jax.random.fold_in(key, 11), (N, N), jnp.float32)
    return (normal_part - normal_part.T) * 0.7071


def block_levels(stream_key, dims, shards, low, top_value):
    level = 1.0
    for axis_at, parts in shards:
        steps = jax.random.uniform(jax.random.fold_in(jax.random.fold_in(stream_key, 6), axis_at), (parts,), jnp.float32, low / len(shards), top_value / len(shards))
        level = level * jnp.repeat(jnp.exp(steps), dims[axis_at] // parts).reshape((-1,) + (1,) * (len(dims) - 1 - axis_at))
    return level


def noise(key, extent, scale, bound, pieces=(), kind=jnp.bfloat16):
    gain = block_levels(key, extent, pieces, -0.22, 0.18) if pieces else 1.0
    drawn = jax.random.normal(key, extent, jnp.float32) * scale * gain
    return jnp.minimum(jnp.maximum(drawn, -bound), bound).astype(kind)


def setup_inputs(seed: int = 0) -> dict:
    arg_keys = jax.random.split(jax.random.key(seed), 5)
    matrix = draw_matrix(jax.random.fold_in(arg_keys[4], 71), 0)
    left_panel = noise(arg_keys[1], (N, K), (K ** -0.25), 2.5, ((0, 16), (1, 16)), jnp.float32)
    right_panel = noise(arg_keys[2], (N, K), (K ** -0.25), 2.5, ((0, 16), (1, 16)), jnp.float32)
    reflectors = noise(arg_keys[3], (N, NB), (N // 4) ** -0.5, 0.109375, ((0, 16), (1, 16)), jnp.float32)
    return {"matrix": matrix, "left_panel": left_panel, "right_panel": right_panel, "reflectors": reflectors}


def product(first, second):
    return jnp.dot(first, second, precision=lax.Precision.HIGHEST, preferred_element_type=jnp.float32)


def reference(matrix, left_panel, right_panel, reflectors):
    reduced = matrix - product(left_panel, right_panel.T) + product(right_panel, left_panel.T)
    image = product(reduced, reflectors)
    return reduced + product(reflectors, image.T) - product(image, reflectors.T)
```

```python
import functools

import jax
import jax.numpy as jnp
from jax import lax
from jax.experimental import pallas as pl
from jax.experimental.pallas import tpu as pltpu
from jax.sharding import PartitionSpec as P

F32 = jnp.float32
BF16 = jnp.bfloat16
MESH = pl.DeviceIdType.MESH

ROW_TREE = {
    (0, 0): (("+", (1, 0)), ("-", (-1, 0)), ("x", (0, 1))),
    (1, 0): (("+", (2, 0)),),
    (-1, 0): (("-", (-2, 0)),),
    (0, 1): (("+", (1, 1)), ("-", (-1, 1))),
    (2, 0): (("+", (3, 0)), ("x", (2, 1))),
    (-2, 0): (("-", (-3, 0)), ("x", (-2, 1))),
    (3, 0): (("+", (4, 0)),),
    (-3, 0): (),
    (1, 1): (),
    (-1, 1): (),
    (2, 1): (("+", (3, 1)),),
    (-2, 1): (("-", (-3, 1)),),
    (4, 0): (("x", (4, 1)),),
    (3, 1): (),
    (-3, 1): (),
    (4, 1): (),
}
COL_TREE = {
    (0, 0, 0): (("+", (1, 0, 0)), ("-", (-1, 0, 0)), ("x", (0, 1, 0)), ("c", (0, 0, 1))),
    (1, 0, 0): (("+", (2, 0, 0)), ("c", (1, 0, 1))),
    (-1, 0, 0): (("c", (-1, 0, 1)),),
    (0, 1, 0): (("+", (1, 1, 0)), ("-", (-1, 1, 0)), ("c", (0, 1, 1))),
    (2, 0, 0): (("c", (2, 0, 1)),),
    (1, 1, 0): (("+", (2, 1, 0)), ("c", (1, 1, 1))),
    (-1, 1, 0): (("c", (-1, 1, 1)),),
    (2, 1, 0): (("c", (2, 1, 1)),),
    (0, 0, 1): (),
    (1, 0, 1): (),
    (-1, 0, 1): (),
    (0, 1, 1): (),
    (2, 0, 1): (),
    (1, 1, 1): (),
    (-1, 1, 1): (),
    (2, 1, 1): (),
}
ROW_SLOTS = tuple(ROW_TREE)
COL_SLOTS = tuple(COL_TREE)
ROW_ID = {slot: n for n, slot in enumerate(ROW_SLOTS)}
COL_ID = {slot: n for n, slot in enumerate(COL_SLOTS)}


def halves(x):
    high = x.astype(BF16)
    return high, (x - high.astype(F32)).astype(BF16)


def dot(a, b, dims):
    return lax.dot_general(a, b, (dims, ((), ())), preferred_element_type=F32)


NT = ((1,), (1,))
NN = ((1,), (0,))


class Place:
    def __init__(self):
        self.i = lax.axis_index("row")
        self.c = lax.axis_index("col")
        self.core = lax.rem(self.i, 2)
        self.y = lax.rem(self.i // 2, 4)
        self.lo = self.i // 8
        self.z = self.c // 2
        self.hi = lax.rem(self.c, 2)
        self.sign = 1 - 2 * self.core

    def row_share(self, slot):
        d, l = slot
        z = lax.rem(self.z - self.sign * d + 8, 8)
        hi = self.hi if l == 0 else 1 - self.hi
        return z * 2 + hi

    def row_target(self, way):
        if way == "x":
            return (self.i, self.z * 2 + 1 - self.hi)
        step = self.sign if way == "+" else -self.sign
        return (self.i, lax.rem(self.z + step + 8, 8) * 2 + self.hi)

    def col_share(self, slot):
        d, l, s = slot
        sign = self.sign if s == 0 else -self.sign
        y = lax.rem(self.y - sign * d + 4, 4)
        lo = self.lo if l == 0 else 1 - self.lo
        core = self.core if s == 0 else 1 - self.core
        return (lo * 4 + y) * 2 + core

    def col_target(self, way):
        if way == "x":
            return (((1 - self.lo) * 4 + self.y) * 2 + self.core, self.c)
        if way == "c":
            return ((self.lo * 4 + self.y) * 2 + 1 - self.core, self.c)
        step = self.sign if way == "+" else -self.sign
        return ((self.lo * 4 + lax.rem(self.y + step + 4, 4)) * 2 + self.core, self.c)


class Gather:
    def __init__(self, place, kind, buf, send, recv, pieces, own):
        self.kind, self.buf, self.send, self.recv = kind, buf, send, recv
        self.pieces, self.own = pieces, own
        self.tree = ROW_TREE if kind == "row" else COL_TREE
        self.ids = ROW_ID if kind == "row" else COL_ID
        self.share = place.row_share if kind == "row" else place.col_share
        self.target = place.row_target if kind == "row" else place.col_target
        self.depth = buf.shape[1] // pieces

    def copy(self, share, way, child, piece, source):
        rows = pl.ds(piece * self.depth, self.depth)
        n = self.ids[child]
        return pltpu.make_async_remote_copy(
            src_ref=source.at[rows],
            dst_ref=self.buf.at[share, rows],
            send_sem=self.send.at[n, piece],
            recv_sem=self.recv.at[n, piece],
            device_id=self.target(way),
            device_id_type=MESH,
        )

    def start(self, slot, piece, ways=None, source=None):
        share = self.share(slot)
        source = self.buf.at[share] if source is None else source
        for way, child in self.tree[slot]:
            if ways is None or way in ways:
                self.copy(share, way, child, piece, source).start()

    def arrive(self, slot, piece):
        rows = pl.ds(piece * self.depth, self.depth)
        part = self.buf.at[self.share(slot), rows]
        n = self.ids[slot]
        pltpu.make_async_copy(part, part, self.recv.at[n, piece]).wait()

    def drain(self):
        root = next(iter(self.tree))
        for slot, n in self.ids.items():
            if slot == root:
                continue
            for piece in range(self.pieces):
                rows = pl.ds(piece * self.depth, self.depth)
                part = self.buf.at[0, rows]
                pltpu.make_async_copy(part, part, self.send.at[n, piece]).wait()


PIECES = 2


def gather_kernel(
    p_ref, q_ref, v_ref, m_ref,
    red, vrow, vcol, wrow, wcol,
    prow, qcol, lhs, rhs, part_row, part_col, got_row, got_col,
    s_p, r_p, s_q, r_q, s_vr, r_vr, s_vc, r_vc, s_wr, r_wr, s_wc, r_wc,
    s_perm, r_perm, s_sum, r_sum,
):
    at = Place()
    i, c = at.i, at.c
    size = m_ref.shape[0]
    tile = 256

    barrier = pltpu.get_barrier_semaphore()
    for n in range(1, 16):
        other = lax.rem(c + n, 16)
        pl.semaphore_signal(barrier, inc=1, device_id=(i, other), device_id_type=MESH)
        other = lax.rem(i + n, 16)
        pl.semaphore_signal(barrier, inc=1, device_id=(other, c), device_id_type=MESH)

    @pl.when(i != c)
    def _():
        pl.semaphore_signal(barrier, inc=1, device_id=(c, i), device_id_type=MESH)
        pl.semaphore_wait(barrier, 31)

    @pl.when(i == c)
    def _():
        pl.semaphore_wait(barrier, 30)

    g_p = Gather(at, "row", prow, s_p, r_p, PIECES, p_ref)
    g_q = Gather(at, "col", qcol, s_q, r_q, PIECES, q_ref)
    g_vr = Gather(at, "row", vrow, s_vr, r_vr, 1, v_ref)
    g_vc = Gather(at, "col", vcol, s_vc, r_vc, 1, v_ref)
    g_wr = Gather(at, "row", wrow, s_wr, r_wr, 1, None)
    g_wc = Gather(at, "col", wcol, s_wc, r_wc, 1, None)

    def crossing(gather, piece, n):
        rows = pl.ds(piece * gather.depth, gather.depth)
        return pltpu.make_async_remote_copy(
            src_ref=gather.own.at[rows],
            dst_ref=gather.buf.at[c, rows],
            send_sem=s_perm.at[n],
            recv_sem=r_perm.at[n],
            device_id=(c, i),
            device_id_type=MESH,
        )

    crossings = [(g_vc, 0, 0)] + [(g_q, piece, 1 + piece) for piece in range(PIECES)]

    g_vr.start((0, 0), 0, source=v_ref)

    @pl.when(i != c)
    def _():
        for args in crossings:
            crossing(*args).start()

    for piece in range(PIECES):
        g_p.start((0, 0), piece, source=p_ref)

    vrow[c] = v_ref[...]
    prow[c] = p_ref[...]

    @pl.when(i == c)
    def _():
        g_vc.start((0, 0, 0), 0, source=v_ref)
        for piece in range(PIECES):
            g_q.start((0, 0, 0), piece, source=q_ref)
        vcol[i] = v_ref[...]
        qcol[i] = q_ref[...]

    def crossed(gather, piece, n):
        @pl.when(i != c)
        def _():
            rows = pl.ds(piece * gather.depth, gather.depth)
            part = gather.buf.at[i, rows]
            pltpu.make_async_copy(part, part, r_perm.at[n]).wait()
            gather.start((0, 0, 0), piece)

    def row_step(gather, slot):
        for piece in range(gather.pieces):
            gather.arrive(slot, piece)
            gather.start(slot, piece)

    def col_step(gather, slot):
        for piece in range(gather.pieces):
            gather.arrive(slot, piece)
            gather.start(slot, piece)

    red[...] = m_ref[...]

    def accumulate(first, second):
        k1, k2 = at.row_share(first), at.row_share(second)
        for n, k in enumerate((k1, k2)):
            high, low = halves(prow[k])
            lhs[:, pl.ds(n * 128, 128)] = high
            lhs[:, pl.ds(256 + n * 128, 128)] = low
            lhs[:, pl.ds(512 + n * 128, 128)] = high
            high, low = halves(qcol[k])
            rhs[:, pl.ds(n * 128, 128)] = high
            rhs[:, pl.ds(256 + n * 128, 128)] = high
            rhs[:, pl.ds(512 + n * 128, 128)] = low

        @pl.loop(0, size // tile)
        def _(t):
            rows = pl.ds(pl.multiple_of(t * tile, tile), tile)
            red[rows, :] += dot(lhs[rows, :], rhs[...], NT)

    for args in crossings:
        crossed(*args)
    for slot in ((0, 1), (1, 0), (-1, 0)):
        row_step(g_vr, slot)
        row_step(g_p, slot)
    for slot in ((0, 0, 1), (1, 0, 0), (-1, 0, 0), (0, 1, 0)):
        col_step(g_vc, slot)
        col_step(g_q, slot)
    for slot in ((2, 0), (-2, 0)):
        row_step(g_vr, slot)
        row_step(g_p, slot)
    for slot in ((2, 0, 0), (1, 1, 0)):
        col_step(g_vc, slot)
        col_step(g_q, slot)
    for slot in ((1, 1), (-1, 1), (3, 0), (-3, 0)):
        row_step(g_vr, slot)
        row_step(g_p, slot)
    for slot in ((-1, 1, 0), (2, 1, 0)):
        col_step(g_vc, slot)
        col_step(g_q, slot)
    for slot in ((2, 1), (-2, 1)):
        row_step(g_vr, slot)
        row_step(g_p, slot)
    for slot in ((1, 0, 1), (-1, 0, 1), (0, 1, 1), (2, 0, 1), (1, 1, 1), (-1, 1, 1), (2, 1, 1)):
        col_step(g_vc, slot)
        col_step(g_q, slot)
    accumulate((0, 0), (0, 1))
    accumulate((1, 0), (-1, 0))
    row_step(g_vr, (4, 0))
    row_step(g_p, (4, 0))
    accumulate((2, 0), (-2, 0))
    accumulate((1, 1), (-1, 1))
    accumulate((3, 0), (-3, 0))
    accumulate((2, 1), (-2, 1))
    for slot in ((3, 1), (-3, 1)):
        row_step(g_vr, slot)
        row_step(g_p, slot)
    accumulate((3, 1), (-3, 1))
    for slot in ((4, 1),):
        row_step(g_vr, slot)
        row_step(g_p, slot)
    accumulate((4, 0), (4, 1))

    high, low = halves(red[...])
    lhs[...] = high
    rhs[...] = low
    width = v_ref.shape[0]
    count = 16 * width
    vh, vl = halves(vcol[...].reshape(count, size))
    part_row[...] = (
        dot(vh, lhs[...], NT) + dot(vh, rhs[...], NT) + dot(vl, lhs[...], NT)
    ).reshape(16, width, size)

    def addend(buf, got, share, target, n):
        return pltpu.make_async_remote_copy(
            src_ref=buf.at[share],
            dst_ref=got.at[n],
            send_sem=s_sum.at[n + (15 if got is got_col else 0)],
            recv_sem=r_sum.at[n + (15 if got is got_col else 0)],
            device_id=target,
            device_id_type=MESH,
        )

    order = (8, 7, 9, 6, 10, 5, 11, 4, 12, 3, 13, 2, 14, 1, 15)
    for n in order:
        other = lax.rem(c + n, 16)
        addend(part_row, got_row, other, (i, other), n - 1).start()
    vh, vl = halves(vrow[...].reshape(count, size))
    part_col[...] = -(
        dot(vh, lhs[...], NN) + dot(vh, rhs[...], NN) + dot(vl, lhs[...], NN)
    ).reshape(16, width, size)
    for n in order:
        other = lax.rem(i + n, 16)
        addend(part_col, got_col, other, (other, c), n - 1).start()

    def gathered(got, n, sem):
        pltpu.make_async_copy(got.at[n], got.at[n], r_sum.at[sem]).wait()

    total = part_col[i]
    for n in range(15):
        gathered(got_col, n, n + 15)
        total += got_col[n]
    wcol[i] = total
    g_wc.start((0, 0, 0), 0)
    total = part_row[c]
    for n in range(15):
        gathered(got_row, n, n)
        total += got_row[n]
    wrow[c] = total
    g_wr.start((0, 0), 0)

    for slot in ((1, 0, 0), (-1, 0, 0), (0, 1, 0)):
        col_step(g_wc, slot)
    for slot in ((1, 0), (-1, 0), (0, 1)):
        row_step(g_wr, slot)
    for slot in ((2, 0, 0), (1, 1, 0), (-1, 1, 0)):
        col_step(g_wc, slot)
    for slot in ((2, 0), (-2, 0), (1, 1), (-1, 1)):
        row_step(g_wr, slot)
    col_step(g_wc, (2, 1, 0))
    for slot in ((3, 0), (-3, 0), (2, 1), (-2, 1)):
        row_step(g_wr, slot)
    for slot in COL_SLOTS[8:]:
        col_step(g_wc, slot)
    for slot in ((4, 0), (3, 1), (-3, 1), (4, 1)):
        row_step(g_wr, slot)

    for gather in (g_p, g_q, g_vr, g_vc, g_wr, g_wc):
        gather.drain()

    @pl.when(i != c)
    def _():
        for gather, piece, n in crossings:
            rows = pl.ds(piece * gather.depth, gather.depth)
            part = gather.own.at[rows]
            pltpu.make_async_copy(part, part, s_perm.at[n]).wait()

    for n in range(30):
        pltpu.make_async_copy(got_row.at[0], got_row.at[0], s_sum.at[n]).wait()


def update_kernel(red, vrow, wrow, vcol, wcol, out, lhs):
    count, size = vrow.shape

    @pl.when(pl.program_id(0) == 0)
    def _():
        for n, ref in enumerate((vrow, wrow)):
            high, low = halves(ref[...].T)
            lhs[:, pl.ds(n * count, count)] = high
            lhs[:, pl.ds((2 + n) * count, count)] = low

    wh, wl = halves(wcol[...])
    vh, vl = halves(-vcol[...])
    high = jnp.concatenate([wh, vh], axis=0)
    low = jnp.concatenate([wl, vl], axis=0)
    first = lhs[:, : 2 * count]
    out[...] = red[...] + (
        dot(first, high, NN) + dot(first, low, NN) + dot(lhs[:, 2 * count :], high, NN)
    )


def local(matrix, left_panel, right_panel, reflectors):
    size = matrix.shape[0]
    width = reflectors.shape[1]
    count = 16 * width
    panel = jnp.concatenate([left_panel, right_panel], axis=1)
    swapped = jnp.concatenate([-right_panel, left_panel], axis=1)
    flat = reflectors.T
    vmem = pl.BlockSpec(memory_space=pltpu.VMEM)
    dma = pltpu.SemaphoreType.DMA
    small = jax.ShapeDtypeStruct((16, width, size), F32)
    sems = [dma((16, PIECES))] * 4 + [dma((16, 1))] * 8 + [dma((1 + PIECES,))] * 2 + [dma((30,))] * 2
    red, vrow, vcol, wrow, wcol = pl.pallas_call(
        gather_kernel,
        name="gather",
        out_shape=(jax.ShapeDtypeStruct((size, size), F32), small, small, small, small),
        in_specs=[vmem] * 4,
        out_specs=(vmem,) * 5,
        scratch_shapes=[
            pltpu.VMEM((16, size, 128), F32),
            pltpu.VMEM((16, size, 128), F32),
            pltpu.VMEM((size, size), BF16),
            pltpu.VMEM((size, size), BF16),
            pltpu.VMEM((16, width, size), F32),
            pltpu.VMEM((16, width, size), F32),
            pltpu.VMEM((15, width, size), F32),
            pltpu.VMEM((15, width, size), F32),
        ]
        + sems,
        compiler_params=pltpu.CompilerParams(
            collective_id=0, has_side_effects=True, vmem_limit_bytes=56 * 1024 * 1024
        ),
    )(panel, swapped, flat, matrix)
    vrow, vcol, wrow, wcol = (x.reshape(count, size) for x in (vrow, vcol, wrow, wcol))
    tile = 256
    whole = pl.BlockSpec((count, size), lambda n: (0, 0))
    strip = pl.BlockSpec((count, tile), lambda n: (0, n))
    block = pl.BlockSpec((size, tile), lambda n: (0, n))
    return pl.pallas_call(
        update_kernel,
        name="update",
        grid=(size // tile,),
        out_shape=jax.ShapeDtypeStruct((size, size), F32),
        in_specs=[block, whole, whole, strip, strip],
        out_specs=block,
        scratch_shapes=[pltpu.VMEM((size, 4 * count), BF16)],
        compiler_params=pltpu.CompilerParams(dimension_semantics=("arbitrary",)),
    )(red, vrow, wrow, vcol, wcol)


def solution(mesh):
    in_specs = (P("row", "col"), P("row", "col"), P("row", "col"), P("row", "col"))
    out_specs = P("row", "col")
    return jax.shard_map(local, mesh=mesh, in_specs=in_specs, out_specs=out_specs, check_vma=False)
```

```python
import functools

import jax
import jax.numpy as jnp
from jax import lax
from jax.experimental import pallas as pl
from jax.experimental.pallas import tpu as pltpu
from jax.sharding import PartitionSpec as P

F32 = jnp.float32
BF16 = jnp.bfloat16
MESH = pl.DeviceIdType.MESH

ROW_TREE = {
    (0, 0): (("+", (1, 0)), ("-", (-1, 0)), ("x", (0, 1))),
    (1, 0): (("+", (2, 0)),),
    (-1, 0): (("-", (-2, 0)),),
    (0, 1): (("+", (1, 1)), ("-", (-1, 1))),
    (2, 0): (("+", (3, 0)), ("x", (2, 1))),
    (-2, 0): (("-", (-3, 0)), ("x", (-2, 1))),
    (3, 0): (("+", (4, 0)),),
    (-3, 0): (),
    (1, 1): (),
    (-1, 1): (),
    (2, 1): (("+", (3, 1)),),
    (-2, 1): (("-", (-3, 1)),),
    (4, 0): (("x", (4, 1)),),
    (3, 1): (),
    (-3, 1): (),
    (4, 1): (),
}
COL_TREE = {
    (0, 0, 0): (("+", (1, 0, 0)), ("-", (-1, 0, 0)), ("x", (0, 1, 0)), ("c", (0, 0, 1))),
    (1, 0, 0): (("+", (2, 0, 0)), ("c", (1, 0, 1))),
    (-1, 0, 0): (("c", (-1, 0, 1)),),
    (0, 1, 0): (("+", (1, 1, 0)), ("-", (-1, 1, 0)), ("c", (0, 1, 1))),
    (2, 0, 0): (("c", (2, 0, 1)),),
    (1, 1, 0): (("+", (2, 1, 0)), ("c", (1, 1, 1))),
    (-1, 1, 0): (("c", (-1, 1, 1)),),
    (2, 1, 0): (("c", (2, 1, 1)),),
    (0, 0, 1): (),
    (1, 0, 1): (),
    (-1, 0, 1): (),
    (0, 1, 1): (),
    (2, 0, 1): (),
    (1, 1, 1): (),
    (-1, 1, 1): (),
    (2, 1, 1): (),
}
ROW_FLAT = {
    (0, 0): (("++", (2, 0)), ("--", (-2, 0)), ("+", (1, 0)), ("-", (-1, 0)), ("x", (0, 1))),
    (1, 0): (("x", (1, 1)),),
    (-1, 0): (("x", (-1, 1)),),
    (0, 1): (),
    (2, 0): (("++", (4, 0)), ("+", (3, 0)), ("x", (2, 1))),
    (-2, 0): (("-", (-3, 0)), ("x", (-2, 1))),
    (3, 0): (("x", (3, 1)),),
    (-3, 0): (("x", (-3, 1)),),
    (1, 1): (),
    (-1, 1): (),
    (2, 1): (),
    (-2, 1): (),
    (4, 0): (("x", (4, 1)),),
    (3, 1): (),
    (-3, 1): (),
    (4, 1): (),
}
COL_FLAT = {
    (0, 0, 0): (("++", (2, 0, 0)), ("+", (1, 0, 0)), ("-", (-1, 0, 0)), ("x", (0, 1, 0)), ("c", (0, 0, 1))),
    (1, 0, 0): (("x", (1, 1, 0)), ("c", (1, 0, 1))),
    (-1, 0, 0): (("x", (-1, 1, 0)), ("c", (-1, 0, 1))),
    (0, 1, 0): (("c", (0, 1, 1)),),
    (2, 0, 0): (("x", (2, 1, 0)), ("c", (2, 0, 1))),
    (1, 1, 0): (("c", (1, 1, 1)),),
    (-1, 1, 0): (("c", (-1, 1, 1)),),
    (2, 1, 0): (("c", (2, 1, 1)),),
    (0, 0, 1): (),
    (1, 0, 1): (),
    (-1, 0, 1): (),
    (0, 1, 1): (),
    (2, 0, 1): (),
    (1, 1, 1): (),
    (-1, 1, 1): (),
    (2, 1, 1): (),
}
STEPS = {"+": 1, "-": -1, "++": 2, "--": -2}
ROW_SLOTS = tuple(ROW_TREE)
COL_SLOTS = tuple(COL_TREE)
ROW_ID = {slot: n for n, slot in enumerate(ROW_SLOTS)}
COL_ID = {slot: n for n, slot in enumerate(COL_SLOTS)}


def halves(x):
    high = x.astype(BF16)
    return high, (x - high.astype(F32)).astype(BF16)


def dot(a, b, dims):
    return lax.dot_general(a, b, (dims, ((), ())), preferred_element_type=F32)


NT = ((1,), (1,))
NN = ((1,), (0,))


class Place:
    def __init__(self):
        self.i = lax.axis_index("row")
        self.c = lax.axis_index("col")
        self.core = lax.rem(self.i, 2)
        self.y = lax.rem(self.i // 2, 4)
        self.lo = self.i // 8
        self.z = self.c // 2
        self.hi = lax.rem(self.c, 2)
        self.sign = 1 - 2 * self.core

    def row_share(self, slot):
        d, l = slot
        z = lax.rem(self.z - self.sign * d + 8, 8)
        hi = self.hi if l == 0 else 1 - self.hi
        return z * 2 + hi

    def row_target(self, way):
        if way == "x":
            return (self.i, self.z * 2 + 1 - self.hi)
        step = self.sign * STEPS[way]
        return (self.i, lax.rem(self.z + step + 8, 8) * 2 + self.hi)

    def col_share(self, slot):
        d, l, s = slot
        sign = self.sign if s == 0 else -self.sign
        y = lax.rem(self.y - sign * d + 4, 4)
        lo = self.lo if l == 0 else 1 - self.lo
        core = self.core if s == 0 else 1 - self.core
        return self.held((lo * 4 + y) * 2 + core, self.c)

    @staticmethod
    def held(i, c):
        core = lax.rem(i, 2)
        return lax.rem(i // 2 - c // 2 - 4 * core + 16, 8) * 2 + core

    def col_target(self, way):
        if way == "x":
            return (((1 - self.lo) * 4 + self.y) * 2 + self.core, self.c)
        if way == "c":
            return ((self.lo * 4 + self.y) * 2 + 1 - self.core, self.c)
        step = self.sign * STEPS[way]
        return ((self.lo * 4 + lax.rem(self.y + step + 4, 4)) * 2 + self.core, self.c)


class Gather:
    def __init__(self, place, kind, tree, buf, send, recv, pieces, own):
        self.kind, self.buf, self.send, self.recv = kind, buf, send, recv
        self.pieces, self.own = pieces, own
        self.tree = tree
        self.ids = ROW_ID if kind == "row" else COL_ID
        self.share = place.row_share if kind == "row" else place.col_share
        self.target = place.row_target if kind == "row" else place.col_target
        self.depth = buf.shape[1] // pieces

    def copy(self, share, way, child, piece, source):
        rows = pl.ds(piece * self.depth, self.depth)
        n = self.ids[child]
        return pltpu.make_async_remote_copy(
            src_ref=source.at[rows],
            dst_ref=self.buf.at[share, rows],
            send_sem=self.send.at[n, piece],
            recv_sem=self.recv.at[n, piece],
            device_id=self.target(way),
            device_id_type=MESH,
        )

    def start(self, slot, piece, ways=None, source=None):
        share = self.share(slot)
        source = self.buf.at[share] if source is None else source
        for way, child in self.tree[slot]:
            if ways is None or way in ways:
                self.copy(share, way, child, piece, source).start()

    def arrive(self, slot, piece):
        rows = pl.ds(piece * self.depth, self.depth)
        part = self.buf.at[self.share(slot), rows]
        n = self.ids[slot]
        pltpu.make_async_copy(part, part, self.recv.at[n, piece]).wait()

    def drain(self):
        root = next(iter(self.tree))
        for slot, n in self.ids.items():
            if slot == root:
                continue
            for piece in range(self.pieces):
                rows = pl.ds(piece * self.depth, self.depth)
                part = self.buf.at[0, rows]
                pltpu.make_async_copy(part, part, self.send.at[n, piece]).wait()


PIECES = 2


def gather_kernel(
    left_ref, right_ref, v_ref, m_ref,
    red, vrow, vcol, wrow, wcol,
    prow, qcol, q_ref, qmid, vmid, lhs, rhs, part_row, part_col, got_row, got_col,
    s_p, r_p, s_q, r_q, s_vr, r_vr, s_vc, r_vc, s_wr, r_wr, s_wc, r_wc,
    s_one, r_one, s_two, r_two, s_sum, r_sum,
):
    at = Place()
    i, c = at.i, at.c
    size = m_ref.shape[0]
    tile = 256

    barrier = pltpu.get_barrier_semaphore()
    for n in range(1, 16):
        other = lax.rem(c + n, 16)
        pl.semaphore_signal(barrier, inc=1, device_id=(i, other), device_id_type=MESH)
        other = lax.rem(i + n, 16)
        pl.semaphore_signal(barrier, inc=1, device_id=(other, c), device_id_type=MESH)

    held = at.held(i, c)
    middle = (lax.rem(at.z + i // 2 + 4 * at.hi, 8) * 2 + at.hi, at.z * 2 + at.core)
    opposite = held // 2
    source = (opposite * 2 + at.hi, at.z * 2 + at.core)
    beyond = (i, opposite * 2 + at.hi)
    moves = jnp.logical_or(at.core != at.hi, lax.rem(at.z + 4 * at.hi, 8) != 0)
    stays = opposite == at.z

    @pl.when(moves)
    def _():
        pl.semaphore_signal(barrier, inc=1, device_id=middle, device_id_type=MESH)
        pl.semaphore_signal(barrier, inc=1, device_id=source, device_id_type=MESH)

    left, right = left_ref[...], right_ref[...]
    q_ref[...] = jnp.concatenate([-right, left], axis=0).T
    prow[c] = jnp.concatenate([left, right], axis=0).T
    vrow[c] = v_ref[...]
    red[...] = m_ref[...]

    @pl.when(moves)
    def _():
        pl.semaphore_wait(barrier, 32)

    @pl.when(jnp.logical_not(moves))
    def _():
        qmid[...] = q_ref[...]
        vmid[...] = v_ref[...]
        pl.semaphore_wait(barrier, 30)

    @pl.when(jnp.logical_and(jnp.logical_not(moves), stays))
    def _():
        qcol[held] = q_ref[...]
        vcol[held] = v_ref[...]

    g_p = Gather(at, "row", ROW_TREE, prow, s_p, r_p, PIECES, None)
    g_q = Gather(at, "col", COL_TREE, qcol, s_q, r_q, PIECES, q_ref)
    g_vr = Gather(at, "row", ROW_FLAT, vrow, s_vr, r_vr, 1, v_ref)
    g_vc = Gather(at, "col", COL_FLAT, vcol, s_vc, r_vc, 1, v_ref)
    g_wr = Gather(at, "row", ROW_FLAT, wrow, s_wr, r_wr, 1, None)
    g_wc = Gather(at, "col", COL_FLAT, wcol, s_wc, r_wc, 1, None)

    crossings = ((g_vc, v_ref, vmid, 0, 0),) + tuple((g_q, q_ref, qmid, n, 1 + n) for n in range(PIECES))

    def first_copy(gather, own, mid, piece, n, direct):
        rows = pl.ds(piece * gather.depth, gather.depth)
        return pltpu.make_async_remote_copy(
            src_ref=own.at[rows],
            dst_ref=gather.buf.at[c, rows] if direct else mid.at[rows],
            send_sem=s_one.at[n],
            recv_sem=r_one.at[n],
            device_id=middle,
            device_id_type=MESH,
        )

    def second_copy(gather, own, mid, piece, n):
        rows = pl.ds(piece * gather.depth, gather.depth)
        return pltpu.make_async_remote_copy(
            src_ref=mid.at[rows],
            dst_ref=gather.buf.at[at.z * 2 + at.core, rows],
            send_sem=s_two.at[n],
            recv_sem=r_two.at[n],
            device_id=beyond,
            device_id_type=MESH,
        )

    g_vr.start((0, 0), 0)

    @pl.when(jnp.logical_and(moves, i // 2 == at.z))
    def _():
        for args in crossings:
            first_copy(*args, True).start()

    @pl.when(jnp.logical_and(moves, i // 2 != at.z))
    def _():
        for args in crossings:
            first_copy(*args, False).start()

    for piece in range(PIECES):
        g_p.start((0, 0), piece)

    def relay(gather, own, mid, piece, n):
        rows = pl.ds(piece * gather.depth, gather.depth)

        @pl.when(moves)
        def _():
            pltpu.make_async_copy(mid.at[rows], mid.at[rows], r_one.at[n]).wait()

        @pl.when(jnp.logical_not(stays))
        def _():
            second_copy(gather, own, mid, piece, n).start()

    def crossed(gather, own, mid, piece, n):
        rows = pl.ds(piece * gather.depth, gather.depth)

        @pl.when(jnp.logical_not(stays))
        def _():
            part = gather.buf.at[held, rows]
            pltpu.make_async_copy(part, part, r_two.at[n]).wait()

        gather.start((0, 0, 0), piece)

    def row_step(gather, slot):
        for piece in range(gather.pieces):
            gather.arrive(slot, piece)
            gather.start(slot, piece)

    def col_step(gather, slot):
        for piece in range(gather.pieces):
            gather.arrive(slot, piece)
            gather.start(slot, piece)

    def accumulate(first, second):
        k1, k2 = at.row_share(first), at.row_share(second)
        for n, k in enumerate((k1, k2)):
            high, low = halves(prow[k])
            lhs[:, pl.ds(n * 128, 128)] = high
            lhs[:, pl.ds(256 + n * 128, 128)] = low
            lhs[:, pl.ds(512 + n * 128, 128)] = high
            high, low = halves(qcol[k])
            rhs[:, pl.ds(n * 128, 128)] = high
            rhs[:, pl.ds(256 + n * 128, 128)] = high
            rhs[:, pl.ds(512 + n * 128, 128)] = low

        @pl.loop(0, size // tile)
        def _(t):
            rows = pl.ds(pl.multiple_of(t * tile, tile), tile)
            red[rows, :] += dot(lhs[rows, :], rhs[...], NT)

    row_step(g_vr, (1, 0))
    row_step(g_vr, (-1, 0))
    for args in crossings:
        relay(*args)
    for slot in ((0, 1), (1, 0), (-1, 0)):
        row_step(g_p, slot)
    for args in crossings:
        crossed(*args)
    for slot in ((2, 0), (-2, 0)):
        row_step(g_vr, slot)
        row_step(g_p, slot)
    row_step(g_vr, (0, 1))
    for slot in ((0, 0, 1), (1, 0, 0), (-1, 0, 0), (0, 1, 0)):
        col_step(g_vc, slot)
        col_step(g_q, slot)
    for slot in ((3, 0), (-3, 0), (1, 1), (-1, 1)):
        row_step(g_vr, slot)
        row_step(g_p, slot)
    for slot in ((2, 0, 0), (1, 1, 0)):
        col_step(g_vc, slot)
        col_step(g_q, slot)
    for slot in ((2, 1), (-2, 1), (4, 0)):
        row_step(g_vr, slot)
        row_step(g_p, slot)
    for slot in ((-1, 1, 0), (2, 1, 0)):
        col_step(g_vc, slot)
        col_step(g_q, slot)
    for slot in ((1, 0, 1), (-1, 0, 1), (0, 1, 1), (2, 0, 1), (1, 1, 1), (-1, 1, 1), (2, 1, 1)):
        col_step(g_vc, slot)
        col_step(g_q, slot)
    accumulate((0, 0), (0, 1))
    accumulate((1, 0), (-1, 0))
    accumulate((2, 0), (-2, 0))
    accumulate((1, 1), (-1, 1))
    accumulate((3, 0), (-3, 0))
    accumulate((2, 1), (-2, 1))
    for slot in ((3, 1), (-3, 1)):
        row_step(g_vr, slot)
        row_step(g_p, slot)
    accumulate((3, 1), (-3, 1))
    for slot in ((4, 1),):
        row_step(g_vr, slot)
        row_step(g_p, slot)
    accumulate((4, 0), (4, 1))

    high, low = halves(red[...])
    lhs[...] = high
    rhs[...] = low
    width = v_ref.shape[0]
    count = 16 * width
    vh, vl = halves(vcol[...].reshape(count, size))
    part_row[...] = (
        dot(vh, lhs[...], NT) + dot(vh, rhs[...], NT) + dot(vl, lhs[...], NT)
    ).reshape(16, width, size)

    def addend(buf, got, share, target, n):
        return pltpu.make_async_remote_copy(
            src_ref=buf.at[share],
            dst_ref=got.at[n],
            send_sem=s_sum.at[n + (15 if got is got_col else 0)],
            recv_sem=r_sum.at[n + (15 if got is got_col else 0)],
            device_id=target,
            device_id_type=MESH,
        )

    order = (8, 7, 9, 6, 10, 5, 11, 4, 12, 3, 13, 2, 14, 1, 15)
    for n in order:
        other = lax.rem(c + n, 16)
        addend(part_row, got_row, other, (i, other), n - 1).start()
    vh, vl = halves(vrow[...].reshape(count, size))
    part_col[...] = -(
        dot(vh, lhs[...], NN) + dot(vh, rhs[...], NN) + dot(vl, lhs[...], NN)
    ).reshape(16, width, size)
    for n in order:
        other = lax.rem(i + n, 16)
        addend(part_col, got_col, at.held(other, c), (other, c), n - 1).start()

    def gathered(got, n, sem):
        pltpu.make_async_copy(got.at[n], got.at[n], r_sum.at[sem]).wait()

    total = part_col[held]
    for n in range(15):
        gathered(got_col, n, n + 15)
        total += got_col[n]
    wcol[held] = total
    g_wc.start((0, 0, 0), 0)
    total = part_row[c]
    for n in range(15):
        gathered(got_row, n, n)
        total += got_row[n]
    wrow[c] = total
    g_wr.start((0, 0), 0)

    for slot in ((0, 0, 1), (1, 0, 0), (-1, 0, 0), (2, 0, 0), (0, 1, 0)):
        col_step(g_wc, slot)
    for slot in ((1, 0), (-1, 0), (2, 0), (-2, 0), (0, 1)):
        row_step(g_wr, slot)
    for slot in ((1, 1, 0), (-1, 1, 0), (2, 1, 0)):
        col_step(g_wc, slot)
    for slot in ((3, 0), (-3, 0), (4, 0), (1, 1), (-1, 1), (2, 1), (-2, 1)):
        row_step(g_wr, slot)
    for slot in COL_SLOTS[9:]:
        col_step(g_wc, slot)
    for slot in ((3, 1), (-3, 1), (4, 1)):
        row_step(g_wr, slot)

    for gather in (g_p, g_q, g_vr, g_vc, g_wr, g_wc):
        gather.drain()

    @pl.when(moves)
    def _():
        for gather, own, mid, piece, n in crossings:
            part = own.at[pl.ds(piece * gather.depth, gather.depth)]
            pltpu.make_async_copy(part, part, s_one.at[n]).wait()

    @pl.when(jnp.logical_not(stays))
    def _():
        for gather, own, mid, piece, n in crossings:
            part = mid.at[pl.ds(piece * gather.depth, gather.depth)]
            pltpu.make_async_copy(part, part, s_two.at[n]).wait()

    for n in range(30):
        pltpu.make_async_copy(got_row.at[0], got_row.at[0], s_sum.at[n]).wait()


def update_kernel(red, vrow, wrow, vcol, wcol, out, lhs):
    count, size = vrow.shape

    @pl.when(pl.program_id(0) == 0)
    def _():
        for n, ref in enumerate((vrow, wrow)):
            high, low = halves(ref[...].T)
            lhs[:, pl.ds(n * count, count)] = high
            lhs[:, pl.ds((2 + n) * count, count)] = low

    wh, wl = halves(wcol[...])
    vh, vl = halves(-vcol[...])
    high = jnp.concatenate([wh, vh], axis=0)
    low = jnp.concatenate([wl, vl], axis=0)
    first = lhs[:, : 2 * count]
    out[...] = red[...] + (
        dot(first, high, NN) + dot(first, low, NN) + dot(lhs[:, 2 * count :], high, NN)
    )


def local(matrix, left_panel, right_panel, reflectors):
    size = matrix.shape[0]
    width = reflectors.shape[1]
    count = 16 * width
    vmem = pl.BlockSpec(memory_space=pltpu.VMEM)
    dma = pltpu.SemaphoreType.DMA
    small = jax.ShapeDtypeStruct((16, width, size), F32)
    sems = [dma((16, PIECES))] * 4 + [dma((16, 1))] * 8 + [dma((1 + PIECES,))] * 4 + [dma((30,))] * 2
    red, vrow, vcol, wrow, wcol = pl.pallas_call(
        gather_kernel,
        name="gather",
        out_shape=(jax.ShapeDtypeStruct((size, size), F32), small, small, small, small),
        in_specs=[vmem] * 4,
        out_specs=(vmem,) * 5,
        scratch_shapes=[
            pltpu.VMEM((16, size, 128), F32),
            pltpu.VMEM((16, size, 128), F32),
            pltpu.VMEM((size, 128), F32),
            pltpu.VMEM((size, 128), F32),
            pltpu.VMEM((width, size), F32),
            pltpu.VMEM((size, size), BF16),
            pltpu.VMEM((size, size), BF16),
            pltpu.VMEM((16, width, size), F32),
            pltpu.VMEM((16, width, size), F32),
            pltpu.VMEM((15, width, size), F32),
            pltpu.VMEM((15, width, size), F32),
        ]
        + sems,
        compiler_params=pltpu.CompilerParams(
            collective_id=0, has_side_effects=True, vmem_limit_bytes=56 * 1024 * 1024
        ),
    )(left_panel.T, right_panel.T, reflectors.T, matrix)
    vrow, vcol, wrow, wcol = (x.reshape(count, size) for x in (vrow, vcol, wrow, wcol))
    tile = 256
    whole = pl.BlockSpec((count, size), lambda n: (0, 0))
    strip = pl.BlockSpec((count, tile), lambda n: (0, n))
    block = pl.BlockSpec((size, tile), lambda n: (0, n))
    return pl.pallas_call(
        update_kernel,
        name="update",
        grid=(size // tile,),
        out_shape=jax.ShapeDtypeStruct((size, size), F32),
        in_specs=[block, whole, whole, strip, strip],
        out_specs=block,
        scratch_shapes=[pltpu.VMEM((size, 4 * count), BF16)],
        compiler_params=pltpu.CompilerParams(dimension_semantics=("arbitrary",)),
    )(red, vrow, wrow, vcol, wcol)


def solution(mesh):
    in_specs = (P("row", "col"), P("row", "col"), P("row", "col"), P("row", "col"))
    out_specs = P("row", "col")
    return jax.shard_map(local, mesh=mesh, in_specs=in_specs, out_specs=out_specs, check_vma=False)
```

```python
import functools

import jax
import jax.numpy as jnp
from jax import lax
from jax.experimental import pallas as pl
from jax.experimental.pallas import tpu as pltpu
from jax.sharding import PartitionSpec as P

F32 = jnp.float32
BF16 = jnp.bfloat16
MESH = pl.DeviceIdType.MESH

ROW_TREE = {
    (0, 0): (("+", (1, 0)), ("-", (-1, 0)), ("x", (0, 1))),
    (1, 0): (("+", (2, 0)),),
    (-1, 0): (("-", (-2, 0)),),
    (0, 1): (("+", (1, 1)), ("-", (-1, 1))),
    (2, 0): (("+", (3, 0)), ("x", (2, 1))),
    (-2, 0): (("-", (-3, 0)), ("x", (-2, 1))),
    (3, 0): (("+", (4, 0)),),
    (-3, 0): (),
    (1, 1): (),
    (-1, 1): (),
    (2, 1): (("+", (3, 1)),),
    (-2, 1): (("-", (-3, 1)),),
    (4, 0): (("x", (4, 1)),),
    (3, 1): (),
    (-3, 1): (),
    (4, 1): (),
}
COL_TREE = {
    (0, 0, 0): (("+", (1, 0, 0)), ("-", (-1, 0, 0)), ("x", (0, 1, 0)), ("c", (0, 0, 1))),
    (1, 0, 0): (("+", (2, 0, 0)), ("c", (1, 0, 1))),
    (-1, 0, 0): (("c", (-1, 0, 1)),),
    (0, 1, 0): (("+", (1, 1, 0)), ("-", (-1, 1, 0)), ("c", (0, 1, 1))),
    (2, 0, 0): (("c", (2, 0, 1)),),
    (1, 1, 0): (("+", (2, 1, 0)), ("c", (1, 1, 1))),
    (-1, 1, 0): (("c", (-1, 1, 1)),),
    (2, 1, 0): (("c", (2, 1, 1)),),
    (0, 0, 1): (),
    (1, 0, 1): (),
    (-1, 0, 1): (),
    (0, 1, 1): (),
    (2, 0, 1): (),
    (1, 1, 1): (),
    (-1, 1, 1): (),
    (2, 1, 1): (),
}
ROW_FLAT = {
    (0, 0): (("++", (2, 0)), ("--", (-2, 0)), ("+", (1, 0)), ("-", (-1, 0)), ("x", (0, 1))),
    (1, 0): (("x", (1, 1)),),
    (-1, 0): (("x", (-1, 1)),),
    (0, 1): (),
    (2, 0): (("++", (4, 0)), ("+", (3, 0)), ("x", (2, 1))),
    (-2, 0): (("-", (-3, 0)), ("x", (-2, 1))),
    (3, 0): (("x", (3, 1)),),
    (-3, 0): (("x", (-3, 1)),),
    (1, 1): (),
    (-1, 1): (),
    (2, 1): (),
    (-2, 1): (),
    (4, 0): (("x", (4, 1)),),
    (3, 1): (),
    (-3, 1): (),
    (4, 1): (),
}
COL_FLAT = {
    (0, 0, 0): (("++", (2, 0, 0)), ("+", (1, 0, 0)), ("-", (-1, 0, 0)), ("x", (0, 1, 0)), ("c", (0, 0, 1))),
    (1, 0, 0): (("x", (1, 1, 0)), ("c", (1, 0, 1))),
    (-1, 0, 0): (("x", (-1, 1, 0)), ("c", (-1, 0, 1))),
    (0, 1, 0): (("c", (0, 1, 1)),),
    (2, 0, 0): (("x", (2, 1, 0)), ("c", (2, 0, 1))),
    (1, 1, 0): (("c", (1, 1, 1)),),
    (-1, 1, 0): (("c", (-1, 1, 1)),),
    (2, 1, 0): (("c", (2, 1, 1)),),
    (0, 0, 1): (),
    (1, 0, 1): (),
    (-1, 0, 1): (),
    (0, 1, 1): (),
    (2, 0, 1): (),
    (1, 1, 1): (),
    (-1, 1, 1): (),
    (2, 1, 1): (),
}
STEPS = {"+": 1, "-": -1, "++": 2, "--": -2}
ROW_SLOTS = tuple(ROW_TREE)
COL_SLOTS = tuple(COL_TREE)
ROW_ID = {slot: n for n, slot in enumerate(ROW_SLOTS)}
COL_ID = {slot: n for n, slot in enumerate(COL_SLOTS)}


def halves(x):
    high = x.astype(BF16)
    return high, (x - high.astype(F32)).astype(BF16)


def dot(a, b, dims):
    return lax.dot_general(a, b, (dims, ((), ())), preferred_element_type=F32)


NT = ((1,), (1,))
NN = ((1,), (0,))


class Place:
    def __init__(self):
        self.i = lax.axis_index("row")
        self.c = lax.axis_index("col")
        self.core = lax.rem(self.i, 2)
        self.y = lax.rem(self.i // 2, 4)
        self.lo = self.i // 8
        self.z = self.c // 2
        self.hi = lax.rem(self.c, 2)
        self.sign = 1 - 2 * self.core

    def row_share(self, slot):
        d, l = slot
        z = lax.rem(self.z - self.sign * d + 8, 8)
        hi = self.hi if l == 0 else 1 - self.hi
        return z * 2 + hi

    def row_target(self, way):
        if way == "x":
            return (self.i, self.z * 2 + 1 - self.hi)
        step = self.sign * STEPS[way]
        return (self.i, lax.rem(self.z + step + 8, 8) * 2 + self.hi)

    def col_share(self, slot):
        d, l, s = slot
        sign = self.sign if s == 0 else -self.sign
        y = lax.rem(self.y - sign * d + 4, 4)
        lo = self.lo if l == 0 else 1 - self.lo
        core = self.core if s == 0 else 1 - self.core
        return self.held((lo * 4 + y) * 2 + core, self.c)

    @staticmethod
    def held(i, c):
        core = lax.rem(i, 2)
        return lax.rem(i // 2 - c // 2 - 4 * core + 16, 8) * 2 + core

    def col_target(self, way):
        if way == "x":
            return (((1 - self.lo) * 4 + self.y) * 2 + self.core, self.c)
        if way == "c":
            return ((self.lo * 4 + self.y) * 2 + 1 - self.core, self.c)
        step = self.sign * STEPS[way]
        return ((self.lo * 4 + lax.rem(self.y + step + 4, 4)) * 2 + self.core, self.c)


class Gather:
    def __init__(self, place, kind, tree, buf, send, recv, pieces, own):
        self.kind, self.buf, self.send, self.recv = kind, buf, send, recv
        self.pieces, self.own = pieces, own
        self.tree = tree
        self.ids = ROW_ID if kind == "row" else COL_ID
        self.share = place.row_share if kind == "row" else place.col_share
        self.target = place.row_target if kind == "row" else place.col_target
        self.depth = buf.shape[1] // pieces

    def copy(self, share, way, child, piece, source):
        rows = pl.ds(piece * self.depth, self.depth)
        n = self.ids[child]
        return pltpu.make_async_remote_copy(
            src_ref=source.at[rows],
            dst_ref=self.buf.at[share, rows],
            send_sem=self.send.at[n, piece],
            recv_sem=self.recv.at[n, piece],
            device_id=self.target(way),
            device_id_type=MESH,
        )

    def start(self, slot, piece, ways=None, source=None):
        share = self.share(slot)
        source = self.buf.at[share] if source is None else source
        for way, child in self.tree[slot]:
            if ways is None or way in ways:
                self.copy(share, way, child, piece, source).start()

    def arrive(self, slot, piece):
        rows = pl.ds(piece * self.depth, self.depth)
        part = self.buf.at[self.share(slot), rows]
        n = self.ids[slot]
        pltpu.make_async_copy(part, part, self.recv.at[n, piece]).wait()

    def drain(self):
        root = next(iter(self.tree))
        for slot, n in self.ids.items():
            if slot == root:
                continue
            for piece in range(self.pieces):
                rows = pl.ds(piece * self.depth, self.depth)
                part = self.buf.at[0, rows]
                pltpu.make_async_copy(part, part, self.send.at[n, piece]).wait()


PIECES = 2


def gather_kernel(
    left_ref, right_ref, v_ref, m_ref,
    red, vrow, vcol, wrow, wcol,
    prow, qcol, q_ref, qmid, vmid, wmid, lhs, rhs, part, paired, got_pair, got,
    s_p, r_p, s_q, r_q, s_vr, r_vr, s_vc, r_vc, s_wr, r_wr, s_wc, r_wc,
    s_one, r_one, s_two, r_two, s_sum, r_sum,
):
    at = Place()
    i, c = at.i, at.c
    size = m_ref.shape[0]
    tile = 256

    barrier = pltpu.get_barrier_semaphore()
    for n in range(1, 16):
        other = lax.rem(c + n, 16)
        pl.semaphore_signal(barrier, inc=1, device_id=(i, other), device_id_type=MESH)
        other = lax.rem(i + n, 16)
        pl.semaphore_signal(barrier, inc=1, device_id=(other, c), device_id_type=MESH)

    held = at.held(i, c)
    middle = (lax.rem(at.z + i // 2 + 4 * at.hi, 8) * 2 + at.hi, at.z * 2 + at.core)
    opposite = held // 2
    source = (opposite * 2 + at.hi, at.z * 2 + at.core)
    beyond = (i, opposite * 2 + at.hi)
    moves = jnp.logical_or(at.core != at.hi, lax.rem(at.z + 4 * at.hi, 8) != 0)
    stays = opposite == at.z

    @pl.when(moves)
    def _():
        pl.semaphore_signal(barrier, inc=1, device_id=middle, device_id_type=MESH)
        pl.semaphore_signal(barrier, inc=1, device_id=source, device_id_type=MESH)

    left, right = left_ref[...], right_ref[...]
    q_ref[...] = jnp.concatenate([-right, left], axis=0).T
    prow[c] = jnp.concatenate([left, right], axis=0).T
    vrow[c] = v_ref[...]
    red[...] = m_ref[...]

    @pl.when(moves)
    def _():
        pl.semaphore_wait(barrier, 32)

    @pl.when(jnp.logical_not(moves))
    def _():
        qmid[...] = q_ref[...]
        vmid[...] = v_ref[...]
        pl.semaphore_wait(barrier, 30)

    @pl.when(jnp.logical_and(jnp.logical_not(moves), stays))
    def _():
        qcol[held] = q_ref[...]
        vcol[held] = v_ref[...]

    g_p = Gather(at, "row", ROW_TREE, prow, s_p, r_p, PIECES, None)
    g_q = Gather(at, "col", COL_TREE, qcol, s_q, r_q, PIECES, q_ref)
    g_vr = Gather(at, "row", ROW_FLAT, vrow, s_vr, r_vr, 1, v_ref)
    g_vc = Gather(at, "col", COL_FLAT, vcol, s_vc, r_vc, 1, v_ref)
    g_wr = Gather(at, "row", ROW_FLAT, wrow, s_wr, r_wr, 1, None)
    g_wc = Gather(at, "col", COL_FLAT, wcol, s_wc, r_wc, 1, None)

    crossings = ((g_vc, v_ref, vmid, 0, 0),) + tuple((g_q, q_ref, qmid, n, 1 + n) for n in range(PIECES))

    def first_copy(gather, own, mid, piece, n, direct):
        rows = pl.ds(piece * gather.depth, gather.depth)
        return pltpu.make_async_remote_copy(
            src_ref=own.at[rows],
            dst_ref=gather.buf.at[c, rows] if direct else mid.at[rows],
            send_sem=s_one.at[n],
            recv_sem=r_one.at[n],
            device_id=middle,
            device_id_type=MESH,
        )

    def second_copy(gather, own, mid, piece, n):
        rows = pl.ds(piece * gather.depth, gather.depth)
        return pltpu.make_async_remote_copy(
            src_ref=mid.at[rows],
            dst_ref=gather.buf.at[at.z * 2 + at.core, rows],
            send_sem=s_two.at[n],
            recv_sem=r_two.at[n],
            device_id=beyond,
            device_id_type=MESH,
        )

    g_vr.start((0, 0), 0)

    @pl.when(jnp.logical_and(moves, i // 2 == at.z))
    def _():
        for args in crossings:
            first_copy(*args, True).start()

    @pl.when(jnp.logical_and(moves, i // 2 != at.z))
    def _():
        for args in crossings:
            first_copy(*args, False).start()

    for piece in range(PIECES):
        g_p.start((0, 0), piece, ways=("+", "-"))

    def relay(gather, own, mid, piece, n):
        rows = pl.ds(piece * gather.depth, gather.depth)

        @pl.when(moves)
        def _():
            pltpu.make_async_copy(mid.at[rows], mid.at[rows], r_one.at[n]).wait()

        @pl.when(jnp.logical_not(stays))
        def _():
            second_copy(gather, own, mid, piece, n).start()

    def crossed(gather, own, mid, piece, n):
        rows = pl.ds(piece * gather.depth, gather.depth)

        @pl.when(jnp.logical_not(stays))
        def _():
            part = gather.buf.at[held, rows]
            pltpu.make_async_copy(part, part, r_two.at[n]).wait()

        gather.start((0, 0, 0), piece)

    def row_step(gather, slot):
        for piece in range(gather.pieces):
            gather.arrive(slot, piece)
            gather.start(slot, piece)

    def col_step(gather, slot):
        for piece in range(gather.pieces):
            gather.arrive(slot, piece)
            gather.start(slot, piece)

    def accumulate(first, second):
        k1, k2 = at.row_share(first), at.row_share(second)
        for n, k in enumerate((k1, k2)):
            high, low = halves(prow[k])
            lhs[:, pl.ds(n * 128, 128)] = high
            lhs[:, pl.ds(256 + n * 128, 128)] = low
            lhs[:, pl.ds(512 + n * 128, 128)] = high
            high, low = halves(qcol[k])
            rhs[:, pl.ds(n * 128, 128)] = high
            rhs[:, pl.ds(256 + n * 128, 128)] = high
            rhs[:, pl.ds(512 + n * 128, 128)] = low

        for t in range(size // tile):
            band = pl.ds(t * tile, tile)
            red[band, :] += dot(lhs[band, :], rhs[...], NT)

    def rows(*slots, v=True, p=True):
        for slot in slots:
            if v:
                row_step(g_vr, slot)
            if p:
                row_step(g_p, slot)

    def cols(*slots):
        for slot in slots:
            col_step(g_vc, slot)
            col_step(g_q, slot)

    rows((1, 0), (-1, 0), p=False)
    for args in crossings:
        relay(*args)
    for piece in range(PIECES):
        g_p.start((0, 0), piece, ways=("x",))
    rows((1, 0), (-1, 0), v=False)
    for args in crossings:
        crossed(*args)
    rows((0, 1), (2, 0), (-2, 0))
    cols((0, 0, 1), (1, 0, 0), (-1, 0, 0), (0, 1, 0))
    rows(*((3, 0),))
    cols(*((2, 0, 0),))
    rows(*((-3, 0),))
    cols((1, 1, 0), (-1, 1, 0))
    rows((1, 1), (-1, 1), (2, 1), (-2, 1), (4, 0))
    cols((2, 1, 0), (1, 0, 1), (-1, 0, 1), (0, 1, 1), (2, 0, 1), (1, 1, 1), (-1, 1, 1), (2, 1, 1))
    accumulate((0, 0), (0, 1))
    accumulate((1, 0), (-1, 0))
    accumulate((2, 0), (-2, 0))
    accumulate((3, 0), (-3, 0))
    accumulate((1, 1), (-1, 1))
    accumulate((2, 1), (-2, 1))
    rows((3, 1), (-3, 1))
    accumulate((3, 1), (-3, 1))
    rows(*((4, 1),))
    accumulate((4, 0), (4, 1))

    high, low = halves(red[...])
    lhs[...] = high
    rhs[...] = low
    width = v_ref.shape[0]
    count = 16 * width
    vh, vl = halves(vrow[...].reshape(count, size))
    part[...] = -(
        dot(vh, lhs[...], NN) + dot(vh, rhs[...], NN) + dot(vl, lhs[...], NN)
    ).reshape(8, 2, width, size)

    pair = pltpu.make_async_remote_copy(
        src_ref=part.at[:, 1 - at.core],
        dst_ref=got_pair,
        send_sem=s_sum.at[7],
        recv_sem=r_sum.at[7],
        device_id=at.col_target("c"),
        device_id_type=MESH,
    )
    pair.start()
    pair.wait_recv()
    paired[...] = part[:, at.core] + got_pair[...]

    def addend(n):
        other = lax.rem(i + 2 * n, 16)
        return pltpu.make_async_remote_copy(
            src_ref=paired.at[at.held(other, c) // 2],
            dst_ref=got.at[n - 1],
            send_sem=s_sum.at[n - 1],
            recv_sem=r_sum.at[n - 1],
            device_id=(other, c),
            device_id_type=MESH,
        )

    for n in (2, 6, 1, 3, 5, 7, 4):
        addend(n).start()
    total = paired[opposite]
    for n in (1, 3, 5, 7, 4, 2, 6):
        addend(n).wait_recv()
        total += got[n - 1]
    wcol[held] = total

    last = 1 + PIECES
    back = pltpu.make_async_remote_copy(
        src_ref=wcol.at[held],
        dst_ref=wmid,
        send_sem=s_two.at[last],
        recv_sem=r_two.at[last],
        device_id=beyond,
        device_id_type=MESH,
    )

    def home(source_ref):
        return pltpu.make_async_remote_copy(
            src_ref=source_ref,
            dst_ref=wrow.at[at.z * 2 + at.core],
            send_sem=s_one.at[last],
            recv_sem=r_one.at[last],
            device_id=source,
            device_id_type=MESH,
        )

    @pl.when(jnp.logical_not(stays))
    def _():
        back.start()

    @pl.when(jnp.logical_and(stays, moves))
    def _():
        home(wcol.at[held]).start()

    @pl.when(jnp.logical_and(stays, jnp.logical_not(moves)))
    def _():
        wrow[c] = wcol[held]

    g_wc.start((0, 0, 0), 0)

    @pl.when(jnp.logical_not(stays))
    def _():
        back.wait_recv()

        @pl.when(moves)
        def _():
            home(wmid).start()

        @pl.when(jnp.logical_not(moves))
        def _():
            wrow[c] = wmid[...]

    for slot in ((1, 0, 0), (-1, 0, 0), (2, 0, 0), (0, 1, 0)):
        col_step(g_wc, slot)

    @pl.when(moves)
    def _():
        pltpu.make_async_copy(wmid, wmid, r_one.at[last]).wait()

    g_wr.start((0, 0), 0)

    for slot in ((1, 1, 0), (-1, 1, 0), (2, 1, 0)):
        col_step(g_wc, slot)
    for slot in ((1, 0), (-1, 0), (2, 0), (-2, 0), (0, 1)):
        row_step(g_wr, slot)
    for slot in ((3, 0), (-3, 0), (4, 0), (1, 1), (-1, 1), (2, 1), (-2, 1)):
        row_step(g_wr, slot)
    for slot in COL_SLOTS[8:]:
        col_step(g_wc, slot)
    for slot in ((3, 1), (-3, 1), (4, 1)):
        row_step(g_wr, slot)

    for gather in (g_p, g_q, g_vr, g_vc, g_wr, g_wc):
        gather.drain()

    @pl.when(moves)
    def _():
        for gather, own, mid, piece, n in crossings:
            part = own.at[pl.ds(piece * gather.depth, gather.depth)]
            pltpu.make_async_copy(part, part, s_one.at[n]).wait()

    @pl.when(jnp.logical_not(stays))
    def _():
        for gather, own, mid, piece, n in crossings:
            part = mid.at[pl.ds(piece * gather.depth, gather.depth)]
            pltpu.make_async_copy(part, part, s_two.at[n]).wait()

    @pl.when(moves)
    def _():
        home(wmid).wait_send()

    @pl.when(jnp.logical_not(stays))
    def _():
        back.wait_send()

    for n in range(1, 8):
        addend(n).wait_send()
    pair.wait_send()


def update_kernel(red, vrow, wrow, vcol, wcol, out, lhs):
    count, size = vrow.shape

    @pl.when(pl.program_id(0) == 0)
    def _():
        for n, ref in enumerate((vrow, wrow)):
            high, low = halves(ref[...].T)
            lhs[:, pl.ds(n * count, count)] = high
            lhs[:, pl.ds((2 + n) * count, count)] = low

    wh, wl = halves(wcol[...])
    vh, vl = halves(-vcol[...])
    high = jnp.concatenate([wh, vh], axis=0)
    low = jnp.concatenate([wl, vl], axis=0)
    first = lhs[:, : 2 * count]
    out[...] = red[...] + (
        dot(first, high, NN) + dot(first, low, NN) + dot(lhs[:, 2 * count :], high, NN)
    )


def local(matrix, left_panel, right_panel, reflectors):
    size = matrix.shape[0]
    width = reflectors.shape[1]
    count = 16 * width
    vmem = pl.BlockSpec(memory_space=pltpu.VMEM)
    dma = pltpu.SemaphoreType.DMA
    small = jax.ShapeDtypeStruct((16, width, size), F32)
    sems = [dma((16, PIECES))] * 4 + [dma((16, 1))] * 8 + [dma((2 + PIECES,))] * 4 + [dma((8,))] * 2
    red, vrow, vcol, wrow, wcol = pl.pallas_call(
        gather_kernel,
        name="gather",
        out_shape=(jax.ShapeDtypeStruct((size, size), F32), small, small, small, small),
        in_specs=[vmem] * 4,
        out_specs=(vmem,) * 5,
        scratch_shapes=[
            pltpu.VMEM((16, size, 128), F32),
            pltpu.VMEM((16, size, 128), F32),
            pltpu.VMEM((size, 128), F32),
            pltpu.VMEM((size, 128), F32),
            pltpu.VMEM((width, size), F32),
            pltpu.VMEM((width, size), F32),
            pltpu.VMEM((size, size), BF16),
            pltpu.VMEM((size, size), BF16),
            pltpu.VMEM((8, 2, width, size), F32),
            pltpu.VMEM((8, width, size), F32),
            pltpu.VMEM((8, width, size), F32),
            pltpu.VMEM((7, width, size), F32),
        ]
        + sems,
        compiler_params=pltpu.CompilerParams(
            collective_id=0, has_side_effects=True, vmem_limit_bytes=56 * 1024 * 1024
        ),
    )(left_panel.T, right_panel.T, reflectors.T, matrix)
    vrow, vcol, wrow, wcol = (x.reshape(count, size) for x in (vrow, vcol, wrow, wcol))
    tile = 256
    whole = pl.BlockSpec((count, size), lambda n: (0, 0))
    strip = pl.BlockSpec((count, tile), lambda n: (0, n))
    block = pl.BlockSpec((size, tile), lambda n: (0, n))
    return pl.pallas_call(
        update_kernel,
        name="update",
        grid=(size // tile,),
        out_shape=jax.ShapeDtypeStruct((size, size), F32),
        in_specs=[block, whole, whole, strip, strip],
        out_specs=block,
        scratch_shapes=[pltpu.VMEM((size, 4 * count), BF16)],
        compiler_params=pltpu.CompilerParams(dimension_semantics=("arbitrary",)),
    )(red, vrow, wrow, vcol, wcol)


def solution(mesh):
    in_specs = (P("row", "col"), P("row", "col"), P("row", "col"), P("row", "col"))
    out_specs = P("row", "col")
    return jax.shard_map(local, mesh=mesh, in_specs=in_specs, out_specs=out_specs, check_vma=False)
```

```python
import functools

import jax
import jax.numpy as jnp
from jax import lax
from jax.experimental import pallas as pl
from jax.experimental.pallas import tpu as pltpu
from jax.sharding import PartitionSpec as P

F32 = jnp.float32
BF16 = jnp.bfloat16
MESH = pl.DeviceIdType.MESH

ROW_TREE = {
    (0, 0): (("+", (1, 0)), ("-", (-1, 0)), ("x", (0, 1))),
    (1, 0): (("+", (2, 0)),),
    (-1, 0): (("-", (-2, 0)),),
    (0, 1): (("+", (1, 1)), ("-", (-1, 1))),
    (2, 0): (("+", (3, 0)), ("x", (2, 1))),
    (-2, 0): (("-", (-3, 0)), ("x", (-2, 1))),
    (3, 0): (("+", (4, 0)),),
    (-3, 0): (),
    (1, 1): (),
    (-1, 1): (),
    (2, 1): (("+", (3, 1)),),
    (-2, 1): (("-", (-3, 1)),),
    (4, 0): (("x", (4, 1)),),
    (3, 1): (),
    (-3, 1): (),
    (4, 1): (),
}
COL_TREE = {
    (0, 0, 0): (("x", (0, 1, 0)), ("+", (1, 0, 0)), ("-", (-1, 0, 0)), ("c", (0, 0, 1))),
    (1, 0, 0): (("+", (2, 0, 0)), ("c", (1, 0, 1))),
    (-1, 0, 0): (("c", (-1, 0, 1)),),
    (0, 1, 0): (("+", (1, 1, 0)), ("-", (-1, 1, 0)), ("c", (0, 1, 1))),
    (2, 0, 0): (("c", (2, 0, 1)),),
    (1, 1, 0): (("+", (2, 1, 0)), ("c", (1, 1, 1))),
    (-1, 1, 0): (("c", (-1, 1, 1)),),
    (2, 1, 0): (("c", (2, 1, 1)),),
    (0, 0, 1): (),
    (1, 0, 1): (),
    (-1, 0, 1): (),
    (0, 1, 1): (),
    (2, 0, 1): (),
    (1, 1, 1): (),
    (-1, 1, 1): (),
    (2, 1, 1): (),
}
ROW_FLAT = {
    (0, 0): (("++", (2, 0)), ("--", (-2, 0)), ("+", (1, 0)), ("-", (-1, 0)), ("x", (0, 1))),
    (1, 0): (("x", (1, 1)),),
    (-1, 0): (("x", (-1, 1)),),
    (0, 1): (),
    (2, 0): (("++", (4, 0)), ("+", (3, 0)), ("x", (2, 1))),
    (-2, 0): (("-", (-3, 0)), ("x", (-2, 1))),
    (3, 0): (("x", (3, 1)),),
    (-3, 0): (("x", (-3, 1)),),
    (1, 1): (),
    (-1, 1): (),
    (2, 1): (),
    (-2, 1): (),
    (4, 0): (("x", (4, 1)),),
    (3, 1): (),
    (-3, 1): (),
    (4, 1): (),
}
COL_FLAT = {
    (0, 0, 0): (("++", (2, 0, 0)), ("+", (1, 0, 0)), ("-", (-1, 0, 0)), ("x", (0, 1, 0)), ("c", (0, 0, 1))),
    (1, 0, 0): (("x", (1, 1, 0)), ("c", (1, 0, 1))),
    (-1, 0, 0): (("x", (-1, 1, 0)), ("c", (-1, 0, 1))),
    (0, 1, 0): (("c", (0, 1, 1)),),
    (2, 0, 0): (("x", (2, 1, 0)), ("c", (2, 0, 1))),
    (1, 1, 0): (("c", (1, 1, 1)),),
    (-1, 1, 0): (("c", (-1, 1, 1)),),
    (2, 1, 0): (("c", (2, 1, 1)),),
    (0, 0, 1): (),
    (1, 0, 1): (),
    (-1, 0, 1): (),
    (0, 1, 1): (),
    (2, 0, 1): (),
    (1, 1, 1): (),
    (-1, 1, 1): (),
    (2, 1, 1): (),
}
STEPS = {"+": 1, "-": -1, "++": 2, "--": -2}
ROW_SLOTS = tuple(ROW_TREE)
COL_SLOTS = tuple(COL_TREE)
ROW_ID = {slot: n for n, slot in enumerate(ROW_SLOTS)}
COL_ID = {slot: n for n, slot in enumerate(COL_SLOTS)}


def halves(x):
    high = x.astype(BF16)
    return high, (x - high.astype(F32)).astype(BF16)


def dot(a, b, dims):
    return lax.dot_general(a, b, (dims, ((), ())), preferred_element_type=F32)


NT = ((1,), (1,))
NN = ((1,), (0,))


class Place:
    def __init__(self):
        self.i = lax.axis_index("row")
        self.c = lax.axis_index("col")
        self.core = lax.rem(self.i, 2)
        self.y = lax.rem(self.i // 2, 4)
        self.lo = self.i // 8
        self.z = self.c // 2
        self.hi = lax.rem(self.c, 2)
        self.sign = 1 - 2 * self.core

    def row_share(self, slot):
        d, l = slot
        z = lax.rem(self.z - self.sign * d + 8, 8)
        hi = self.hi if l == 0 else 1 - self.hi
        return z * 2 + hi

    def row_target(self, way):
        if way == "x":
            return (self.i, self.z * 2 + 1 - self.hi)
        step = self.sign * STEPS[way]
        return (self.i, lax.rem(self.z + step + 8, 8) * 2 + self.hi)

    def col_share(self, slot):
        d, l, s = slot
        sign = self.sign if s == 0 else -self.sign
        y = lax.rem(self.y - sign * d + 4, 4)
        lo = self.lo if l == 0 else 1 - self.lo
        core = self.core if s == 0 else 1 - self.core
        return self.held((lo * 4 + y) * 2 + core, self.c)

    @staticmethod
    def held(i, c):
        core = lax.rem(i, 2)
        return lax.rem(i // 2 - c // 2 - 4 * core + 16, 8) * 2 + core

    @staticmethod
    def holder(share, c):
        core = lax.rem(share, 2)
        return lax.rem(c // 2 + share // 2 + 4 * core, 8) * 2 + core

    def col_target(self, way):
        if way == "x":
            return (((1 - self.lo) * 4 + self.y) * 2 + self.core, self.c)
        if way == "c":
            return ((self.lo * 4 + self.y) * 2 + 1 - self.core, self.c)
        step = self.sign * STEPS[way]
        return ((self.lo * 4 + lax.rem(self.y + step + 4, 4)) * 2 + self.core, self.c)


class Gather:
    def __init__(self, place, kind, tree, buf, send, recv, pieces, own):
        self.kind, self.buf, self.send, self.recv = kind, buf, send, recv
        self.pieces, self.own = pieces, own
        self.tree = tree
        self.ids = ROW_ID if kind == "row" else COL_ID
        self.share = place.row_share if kind == "row" else place.col_share
        self.target = place.row_target if kind == "row" else place.col_target
        self.depth = buf.shape[1] // pieces

    def copy(self, share, way, child, piece, source):
        rows = pl.ds(piece * self.depth, self.depth)
        n = self.ids[child]
        return pltpu.make_async_remote_copy(
            src_ref=source.at[rows],
            dst_ref=self.buf.at[share, rows],
            send_sem=self.send.at[n, piece],
            recv_sem=self.recv.at[n, piece],
            device_id=self.target(way),
            device_id_type=MESH,
        )

    def start(self, slot, piece, ways=None, source=None):
        share = self.share(slot)
        source = self.buf.at[share] if source is None else source
        for way, child in self.tree[slot]:
            if ways is None or way in ways:
                self.copy(share, way, child, piece, source).start()

    def arrive(self, slot, piece):
        rows = pl.ds(piece * self.depth, self.depth)
        part = self.buf.at[self.share(slot), rows]
        n = self.ids[slot]
        pltpu.make_async_copy(part, part, self.recv.at[n, piece]).wait()

    def drain(self):
        root = next(iter(self.tree))
        for slot, n in self.ids.items():
            if slot == root:
                continue
            for piece in range(self.pieces):
                rows = pl.ds(piece * self.depth, self.depth)
                part = self.buf.at[0, rows]
                pltpu.make_async_copy(part, part, self.send.at[n, piece]).wait()


PIECES = 2


def gather_kernel(
    left_ref, right_ref, v_ref, m_ref,
    red,
    vrow, vcol, wrow, wcol, rhs2, prow, qcol, q_ref, qmid, vmid, wmid, lhs, rhs, part, paired, got_pair, got, tpart, tsum, tpair, tgot, tall, town,
    s_p, r_p, s_q, r_q, s_vr, r_vr, s_vc, r_vc, s_wr, r_wr, s_wc, r_wc,
    s_one, r_one, s_two, r_two, s_sum, r_sum, s_t, r_t, s_all, r_all,
):
    at = Place()
    i, c = at.i, at.c
    size = m_ref.shape[0]
    tile = 256

    barrier = pltpu.get_barrier_semaphore()
    held = at.held(i, c)
    middle = (lax.rem(at.z + i // 2 + 4 * at.hi, 8) * 2 + at.hi, at.z * 2 + at.core)
    opposite = held // 2
    source = (opposite * 2 + at.hi, at.z * 2 + at.core)
    beyond = (i, opposite * 2 + at.hi)
    moves = jnp.logical_or(at.core != at.hi, lax.rem(at.z + 4 * at.hi, 8) != 0)
    stays = opposite == at.z

    def greet(device):
        pl.semaphore_signal(barrier, inc=1, device_id=device, device_id_type=MESH)

    @pl.when(jnp.logical_not(stays))
    def _():
        greet(beyond)

    @pl.when(moves)
    def _():
        greet(middle)
        greet(source)

    for way in ("++", "--", "x", "+", "-"):
        greet(at.row_target(way))
    for n in range(1, 8):
        greet((lax.rem(i + 2 * n, 16), c))
    greet(at.col_target("c"))
    for n in range(1, 16):
        j = lax.rem(c + n, 16)
        greet((at.holder(c, j), j))
        greet((lax.rem(i + n, 16), held))

    @pl.when(held != c)
    def _():
        greet((at.holder(c, c), c))
        greet((i, held))

    left, right = left_ref[...], right_ref[...]
    q_ref[...] = jnp.concatenate([-right, left], axis=0).T
    prow[c] = jnp.concatenate([left, right], axis=0).T
    vrow[c] = v_ref[...]
    red[...] = m_ref[...]

    @pl.when(jnp.logical_not(moves))
    def _():
        qmid[...] = q_ref[...]
        vmid[...] = v_ref[...]

    peers = 43 + jnp.where(held != c, 2, 0) + jnp.where(stays, 0, 1) + jnp.where(moves, 2, 0)
    pl.semaphore_wait(barrier, peers)

    @pl.when(jnp.logical_and(jnp.logical_not(moves), stays))
    def _():
        qcol[held] = q_ref[...]
        vcol[held] = v_ref[...]

    g_p = Gather(at, "row", ROW_TREE, prow, s_p, r_p, PIECES, None)
    g_q = Gather(at, "col", COL_TREE, qcol, s_q, r_q, PIECES, q_ref)
    g_vr = Gather(at, "row", ROW_FLAT, vrow, s_vr, r_vr, 1, v_ref)
    g_vc = Gather(at, "col", COL_FLAT, vcol, s_vc, r_vc, 1, v_ref)
    g_wr = Gather(at, "row", ROW_FLAT, wrow, s_wr, r_wr, 1, None)
    g_wc = Gather(at, "col", COL_FLAT, wcol, s_wc, r_wc, 1, None)

    crossings = ((g_vc, v_ref, vmid, 0, 0),) + tuple((g_q, q_ref, qmid, n, 1 + n) for n in range(PIECES))

    def first_copy(gather, own, mid, piece, n, direct):
        rows = pl.ds(piece * gather.depth, gather.depth)
        return pltpu.make_async_remote_copy(
            src_ref=own.at[rows],
            dst_ref=gather.buf.at[c, rows] if direct else mid.at[rows],
            send_sem=s_one.at[n],
            recv_sem=r_one.at[n],
            device_id=middle,
            device_id_type=MESH,
        )

    def second_copy(gather, own, mid, piece, n):
        rows = pl.ds(piece * gather.depth, gather.depth)
        return pltpu.make_async_remote_copy(
            src_ref=mid.at[rows],
            dst_ref=gather.buf.at[at.z * 2 + at.core, rows],
            send_sem=s_two.at[n],
            recv_sem=r_two.at[n],
            device_id=beyond,
            device_id_type=MESH,
        )

    g_vr.start((0, 0), 0)

    @pl.when(jnp.logical_and(moves, i // 2 == at.z))
    def _():
        for args in crossings:
            first_copy(*args, True).start()

    @pl.when(jnp.logical_and(moves, i // 2 != at.z))
    def _():
        for args in crossings:
            first_copy(*args, False).start()

    for piece in range(PIECES):
        g_p.start((0, 0), piece, ways=("+", "-"))

    def relay(gather, own, mid, piece, n):
        rows = pl.ds(piece * gather.depth, gather.depth)

        @pl.when(moves)
        def _():
            pltpu.make_async_copy(mid.at[rows], mid.at[rows], r_one.at[n]).wait()

        @pl.when(jnp.logical_not(stays))
        def _():
            second_copy(gather, own, mid, piece, n).start()

    def crossed(gather, own, mid, piece, n):
        rows = pl.ds(piece * gather.depth, gather.depth)

        @pl.when(jnp.logical_not(stays))
        def _():
            part = gather.buf.at[held, rows]
            pltpu.make_async_copy(part, part, r_two.at[n]).wait()

        gather.start((0, 0, 0), piece)

    def row_step(gather, slot):
        for piece in range(gather.pieces):
            gather.arrive(slot, piece)
            gather.start(slot, piece)

    def col_step(gather, slot):
        for piece in range(gather.pieces):
            gather.arrive(slot, piece)
            gather.start(slot, piece)

    def accumulate(first, second):
        k1, k2 = at.row_share(first), at.row_share(second)
        for n, k in enumerate((k1, k2)):
            high, low = halves(prow[k])
            lhs[:, pl.ds(n * 128, 128)] = high
            lhs[:, pl.ds(256 + n * 128, 128)] = low
            lhs[:, pl.ds(512 + n * 128, 128)] = high
            high, low = halves(qcol[k])
            rhs[:, pl.ds(n * 128, 128)] = high
            rhs[:, pl.ds(256 + n * 128, 128)] = high
            rhs[:, pl.ds(512 + n * 128, 128)] = low

        for t in range(size // tile):
            band = pl.ds(t * tile, tile)
            red[band, :] += dot(lhs[band, :], rhs[...], NT)

    def run(step, gather, *slots):
        for slot in slots:
            step(gather, slot)

    width = v_ref.shape[0]
    count = 16 * width
    sibling = at.col_target("c")

    def factor():
        vh, vl = halves(vrow[...].reshape(count, size))
        ph, pl_ = halves(prow[c])
        tpart[...] = (dot(vh, ph, NN) + dot(vh, pl_, NN) + dot(vl, ph, NN)).reshape(8, 2, width, 128)
        tpaired().start()

    def image_first():
        vh, vl = halves(vrow[...].reshape(count, size))
        high, low = halves(m_ref[...])
        lhs[...] = high
        rhs[...] = low
        part[...] = (
            dot(vh, lhs[...], NN) + dot(vh, rhs[...], NN) + dot(vl, lhs[...], NN)
        ).reshape(8, 2, width, size)

    def tpaired():
        return pltpu.make_async_remote_copy(
            src_ref=tpart.at[:, 1 - at.core],
            dst_ref=tpair,
            send_sem=s_t.at[7],
            recv_sem=r_t.at[7],
            device_id=sibling,
            device_id_type=MESH,
        )

    def taddend(n):
        other = lax.rem(i + 2 * n, 16)
        return pltpu.make_async_remote_copy(
            src_ref=tsum.at[other // 2],
            dst_ref=tgot.at[n - 1],
            send_sem=s_t.at[n - 1],
            recv_sem=r_t.at[n - 1],
            device_id=(other, c),
            device_id_type=MESH,
        )

    def factor_sums():
        tpaired().wait_recv()
        tsum[...] = tpart[:, at.core] + tpair[...]
        for n in (2, 6, 1, 3, 5, 7, 4):
            taddend(n).start()

    def tspread(n):
        j = lax.rem(c + n, 16)
        return pltpu.make_async_remote_copy(
            src_ref=town,
            dst_ref=tall.at[i],
            send_sem=s_all.at[n],
            recv_sem=r_all.at[i],
            device_id=(at.holder(c, j), j),
            device_id_type=MESH,
        )

    def factor_spread():
        total = tsum[i // 2]
        for n in (1, 3, 5, 7, 4, 2, 6):
            taddend(n).wait_recv()
            total += tgot[n - 1]
        town[...] = total

        @pl.when(held != c)
        def _():
            tspread(0).start()

        @pl.when(held == c)
        def _():
            tall[i] = town[...]

        for n in (8, 7, 9, 6, 10, 5, 11, 4, 12, 3, 13, 2, 14, 1, 15):
            tspread(n).start()

    def from_row(n):
        row = lax.rem(i + n, 16)
        pltpu.make_async_copy(tall.at[row], tall.at[row], r_all.at[row]).wait()

    def image():
        for n in range(1, 16):
            from_row(n)

        @pl.when(held != c)
        def _():
            from_row(0)

        th, tl = halves(tall[...].reshape(count, 128))
        qh, ql = halves(qcol[held])
        more = dot(th, qh, NT) + dot(th, ql, NT) + dot(tl, qh, NT)
        part[...] = -(part[...] + more.reshape(8, 2, width, size))
        paired_copy().start()

    def paired_copy():
        return pltpu.make_async_remote_copy(
            src_ref=part.at[:, 1 - at.core],
            dst_ref=got_pair,
            send_sem=s_sum.at[7],
            recv_sem=r_sum.at[7],
            device_id=sibling,
            device_id_type=MESH,
        )

    def addend(n):
        other = lax.rem(i + 2 * n, 16)
        return pltpu.make_async_remote_copy(
            src_ref=paired.at[at.held(other, c) // 2],
            dst_ref=got.at[n - 1],
            send_sem=s_sum.at[n - 1],
            recv_sem=r_sum.at[n - 1],
            device_id=(other, c),
            device_id_type=MESH,
        )

    def image_sums():
        paired_copy().wait_recv()
        paired[...] = part[:, at.core] + got_pair[...]
        for n in (2, 6, 1, 3, 5, 7, 4):
            addend(n).start()

    last = 1 + PIECES
    back = pltpu.make_async_remote_copy(
        src_ref=wcol.at[held],
        dst_ref=wmid,
        send_sem=s_two.at[last],
        recv_sem=r_two.at[last],
        device_id=beyond,
        device_id_type=MESH,
    )

    def home(source_ref):
        return pltpu.make_async_remote_copy(
            src_ref=source_ref,
            dst_ref=wrow.at[at.z * 2 + at.core],
            send_sem=s_one.at[last],
            recv_sem=r_one.at[last],
            device_id=source,
            device_id_type=MESH,
        )

    def image_share():
        total = paired[opposite]
        for n in (1, 3, 5, 7, 4, 2, 6):
            addend(n).wait_recv()
            total += got[n - 1]
        wcol[held] = total

        @pl.when(jnp.logical_not(stays))
        def _():
            back.start()

        @pl.when(jnp.logical_and(stays, moves))
        def _():
            home(wcol.at[held]).start()

        @pl.when(jnp.logical_and(stays, jnp.logical_not(moves)))
        def _():
            wrow[c] = wcol[held]

        g_wc.start((0, 0, 0), 0)

    def image_back():
        @pl.when(jnp.logical_not(stays))
        def _():
            back.wait_recv()

            @pl.when(moves)
            def _():
                home(wmid).start()

            @pl.when(jnp.logical_not(moves))
            def _():
                wrow[c] = wmid[...]

    def image_home():
        @pl.when(moves)
        def _():
            pltpu.make_async_copy(wmid, wmid, r_one.at[last]).wait()

        g_wr.start((0, 0), 0)

    def stage(target, flat):
        high, low = halves(flat)
        target[:count] = high
        target[count : 2 * count] = high
        target[2 * count :] = low

    def outer(rows_ref, right):
        high, low = halves(rows_ref[...].reshape(count, size).T)
        lhs[:, :count] = high
        lhs[:, count : 2 * count] = low
        lhs[:, 2 * count :] = high
        for t in range(size // tile):
            band = pl.ds(t * tile, tile)
            red[band, :] += dot(lhs[band, :], right[...], NN)

    def first_outer():
        stage(rhs, wcol[...].reshape(count, size))
        outer(vrow, rhs)
        stage(rhs2, -vcol[...].reshape(count, size))

    def last_outer():
        outer(wrow, rhs2)

    far = lax.rem(opposite - at.z + 8, 8) == 4

    for args in crossings[:1]:
        relay(*args)
    run(row_step, g_vr, (2, 0), (-2, 0), (1, 0), (-1, 0))
    for args in crossings[1:]:
        relay(*args)
    run(row_step, g_vr, (3, 0), (-3, 0), (4, 0))
    run(row_step, g_p, (1, 0), (-1, 0))
    for piece in range(PIECES):
        g_p.start((0, 0), piece, ways=("x",))

    @pl.when(jnp.logical_not(far))
    def _():
        for args in crossings:
            crossed(*args)

    run(row_step, g_vr, (0, 1), (1, 1), (-1, 1), (2, 1), (-2, 1), (3, 1), (-3, 1), (4, 1))
    factor()
    factor_sums()

    @pl.when(far)
    def _():
        for args in crossings:
            crossed(*args)

    image_first()
    run(col_step, g_q, (1, 0, 0), (-1, 0, 0), (0, 1, 0))
    run(row_step, g_p, (0, 1))
    factor_spread()
    run(row_step, g_p, (2, 0), (-2, 0))
    run(col_step, g_vc, (1, 0, 0), (-1, 0, 0), (2, 0, 0))
    run(col_step, g_q, (1, 1, 0), (-1, 1, 0), (2, 0, 0))
    image()
    run(row_step, g_p, (3, 0), (-3, 0))
    image_sums()
    run(row_step, g_p, (2, 1), (-2, 1))
    run(row_step, g_p, (4, 0))
    run(col_step, g_q, (2, 1, 0))
    run(col_step, g_vc, (0, 1, 0), (1, 1, 0), (-1, 1, 0), (2, 1, 0))
    run(col_step, g_q, *COL_SLOTS[8:])
    run(row_step, g_p, (1, 1), (-1, 1))
    accumulate((0, 0), (0, 1))
    image_share()
    accumulate((1, 0), (-1, 0))
    accumulate((2, 0), (-2, 0))
    accumulate((3, 0), (-3, 0))
    image_back()
    accumulate((1, 1), (-1, 1))
    accumulate((2, 1), (-2, 1))
    run(col_step, g_wc, (1, 0, 0), (-1, 0, 0), (2, 0, 0), (0, 1, 0))
    image_home()
    run(row_step, g_p, (3, 1), (-3, 1))
    run(row_step, g_wr, (1, 0), (-1, 0), (2, 0), (-2, 0))
    accumulate((3, 1), (-3, 1))
    run(col_step, g_wc, (1, 1, 0), (-1, 1, 0), (2, 1, 0))
    run(row_step, g_p, (4, 1))
    run(row_step, g_wr, (3, 0), (-3, 0), (4, 0))
    accumulate((4, 0), (4, 1))
    run(col_step, g_vc, *COL_SLOTS[8:])
    run(col_step, g_wc, *COL_SLOTS[8:])
    first_outer()
    run(row_step, g_wr, (0, 1), (1, 1), (-1, 1), (2, 1), (-2, 1), (3, 1), (-3, 1), (4, 1))
    last_outer()

    for gather in (g_p, g_q, g_vr, g_vc, g_wr, g_wc):
        gather.drain()

    @pl.when(moves)
    def _():
        for gather, own, mid, piece, n in crossings:
            part = own.at[pl.ds(piece * gather.depth, gather.depth)]
            pltpu.make_async_copy(part, part, s_one.at[n]).wait()

    @pl.when(jnp.logical_not(stays))
    def _():
        for gather, own, mid, piece, n in crossings:
            part = mid.at[pl.ds(piece * gather.depth, gather.depth)]
            pltpu.make_async_copy(part, part, s_two.at[n]).wait()

    @pl.when(moves)
    def _():
        home(wmid).wait_send()

    @pl.when(jnp.logical_not(stays))
    def _():
        back.wait_send()

    @pl.when(held != c)
    def _():
        tspread(0).wait_send()

    for n in range(1, 16):
        tspread(n).wait_send()
    for n in range(1, 8):
        addend(n).wait_send()
        taddend(n).wait_send()
    paired_copy().wait_send()
    tpaired().wait_send()


def local(matrix, left_panel, right_panel, reflectors):
    size = matrix.shape[0]
    width = reflectors.shape[1]
    vmem = pl.BlockSpec(memory_space=pltpu.VMEM)
    dma = pltpu.SemaphoreType.DMA
    sems = [dma((16, PIECES))] * 4 + [dma((16, 1))] * 8 + [dma((2 + PIECES,))] * 4 + [dma((8,))] * 4 + [dma((16,))] * 2
    return pl.pallas_call(
        gather_kernel,
        name="gather",
        out_shape=jax.ShapeDtypeStruct((size, size), F32),
        in_specs=[vmem] * 4,
        out_specs=vmem,
        scratch_shapes=[pltpu.VMEM((16, width, size), F32)] * 4
        + [
            pltpu.VMEM((size, size), BF16),
            pltpu.VMEM((16, size, 128), F32),
            pltpu.VMEM((16, size, 128), F32),
            pltpu.VMEM((size, 128), F32),
            pltpu.VMEM((size, 128), F32),
            pltpu.VMEM((width, size), F32),
            pltpu.VMEM((width, size), F32),
            pltpu.VMEM((size, size), BF16),
            pltpu.VMEM((size, size), BF16),
            pltpu.VMEM((8, 2, width, size), F32),
            pltpu.VMEM((8, width, size), F32),
            pltpu.VMEM((8, width, size), F32),
            pltpu.VMEM((7, width, size), F32),
            pltpu.VMEM((8, 2, width, 128), F32),
            pltpu.VMEM((8, width, 128), F32),
            pltpu.VMEM((8, width, 128), F32),
            pltpu.VMEM((7, width, 128), F32),
            pltpu.VMEM((16, width, 128), F32),
            pltpu.VMEM((width, 128), F32),
        ]
        + sems,
        compiler_params=pltpu.CompilerParams(
            collective_id=0, has_side_effects=True, vmem_limit_bytes=56 * 1024 * 1024
        ),
    )(left_panel.T, right_panel.T, reflectors.T, matrix)


def solution(mesh):
    in_specs = (P("row", "col"), P("row", "col"), P("row", "col"), P("row", "col"))
    out_specs = P("row", "col")
    return jax.shard_map(local, mesh=mesh, in_specs=in_specs, out_specs=out_specs, check_vma=False)
```

```python
import functools

import jax
import jax.numpy as jnp
from jax import lax
from jax.experimental import pallas as pl
from jax.experimental.pallas import tpu as pltpu
from jax.sharding import PartitionSpec as P

F32 = jnp.float32
BF16 = jnp.bfloat16
MESH = pl.DeviceIdType.MESH

ROW_TREE = {
    (0, 0): (("+", (1, 0)), ("-", (-1, 0)), ("x", (0, 1))),
    (1, 0): (("+", (2, 0)),),
    (-1, 0): (("-", (-2, 0)),),
    (0, 1): (("+", (1, 1)), ("-", (-1, 1))),
    (2, 0): (("+", (3, 0)), ("x", (2, 1))),
    (-2, 0): (("-", (-3, 0)), ("x", (-2, 1))),
    (3, 0): (("+", (4, 0)),),
    (-3, 0): (),
    (1, 1): (),
    (-1, 1): (),
    (2, 1): (("+", (3, 1)),),
    (-2, 1): (("-", (-3, 1)),),
    (4, 0): (("x", (4, 1)),),
    (3, 1): (),
    (-3, 1): (),
    (4, 1): (),
}
COL_TREE = {
    (0, 0, 0): (("x", (0, 1, 0)), ("+", (1, 0, 0)), ("-", (-1, 0, 0)), ("c", (0, 0, 1))),
    (1, 0, 0): (("+", (2, 0, 0)), ("c", (1, 0, 1))),
    (-1, 0, 0): (("c", (-1, 0, 1)),),
    (0, 1, 0): (("+", (1, 1, 0)), ("-", (-1, 1, 0)), ("c", (0, 1, 1))),
    (2, 0, 0): (("c", (2, 0, 1)),),
    (1, 1, 0): (("+", (2, 1, 0)), ("c", (1, 1, 1))),
    (-1, 1, 0): (("c", (-1, 1, 1)),),
    (2, 1, 0): (("c", (2, 1, 1)),),
    (0, 0, 1): (),
    (1, 0, 1): (),
    (-1, 0, 1): (),
    (0, 1, 1): (),
    (2, 0, 1): (),
    (1, 1, 1): (),
    (-1, 1, 1): (),
    (2, 1, 1): (),
}
ROW_FLAT = {
    (0, 0): (("++", (2, 0)), ("--", (-2, 0)), ("+", (1, 0)), ("-", (-1, 0)), ("x", (0, 1))),
    (1, 0): (("x", (1, 1)),),
    (-1, 0): (("x", (-1, 1)),),
    (0, 1): (),
    (2, 0): (("++", (4, 0)), ("+", (3, 0)), ("x", (2, 1))),
    (-2, 0): (("-", (-3, 0)), ("x", (-2, 1))),
    (3, 0): (("x", (3, 1)),),
    (-3, 0): (("x", (-3, 1)),),
    (1, 1): (),
    (-1, 1): (),
    (2, 1): (),
    (-2, 1): (),
    (4, 0): (("x", (4, 1)),),
    (3, 1): (),
    (-3, 1): (),
    (4, 1): (),
}
COL_FLAT = {
    (0, 0, 0): (("++", (2, 0, 0)), ("+", (1, 0, 0)), ("-", (-1, 0, 0)), ("x", (0, 1, 0)), ("c", (0, 0, 1))),
    (1, 0, 0): (("x", (1, 1, 0)), ("c", (1, 0, 1))),
    (-1, 0, 0): (("x", (-1, 1, 0)), ("c", (-1, 0, 1))),
    (0, 1, 0): (("c", (0, 1, 1)),),
    (2, 0, 0): (("x", (2, 1, 0)), ("c", (2, 0, 1))),
    (1, 1, 0): (("c", (1, 1, 1)),),
    (-1, 1, 0): (("c", (-1, 1, 1)),),
    (2, 1, 0): (("c", (2, 1, 1)),),
    (0, 0, 1): (),
    (1, 0, 1): (),
    (-1, 0, 1): (),
    (0, 1, 1): (),
    (2, 0, 1): (),
    (1, 1, 1): (),
    (-1, 1, 1): (),
    (2, 1, 1): (),
}
STEPS = {"+": 1, "-": -1, "++": 2, "--": -2}
ROW_SLOTS = tuple(ROW_TREE)
COL_SLOTS = tuple(COL_TREE)
ROW_ID = {slot: n for n, slot in enumerate(ROW_SLOTS)}
COL_ID = {slot: n for n, slot in enumerate(COL_SLOTS)}


def halves(x):
    high = x.astype(BF16)
    return high, (x - high.astype(F32)).astype(BF16)


def dot(a, b, dims):
    return lax.dot_general(a, b, (dims, ((), ())), preferred_element_type=F32)


NT = ((1,), (1,))
NN = ((1,), (0,))


class Place:
    def __init__(self):
        self.i = lax.axis_index("row")
        self.c = lax.axis_index("col")
        self.core = lax.rem(self.i, 2)
        self.y = lax.rem(self.i // 2, 4)
        self.lo = self.i // 8
        self.z = self.c // 2
        self.hi = lax.rem(self.c, 2)
        self.sign = 1 - 2 * self.core

    def row_share(self, slot):
        d, l = slot
        z = lax.rem(self.z - self.sign * d + 8, 8)
        hi = self.hi if l == 0 else 1 - self.hi
        return z * 2 + hi

    def row_target(self, way):
        if way == "x":
            return (self.i, self.z * 2 + 1 - self.hi)
        step = self.sign * STEPS[way]
        return (self.i, lax.rem(self.z + step + 8, 8) * 2 + self.hi)

    def col_share(self, slot):
        d, l, s = slot
        sign = self.sign if s == 0 else -self.sign
        y = lax.rem(self.y - sign * d + 4, 4)
        lo = self.lo if l == 0 else 1 - self.lo
        core = self.core if s == 0 else 1 - self.core
        return self.held((lo * 4 + y) * 2 + core, self.c)

    @staticmethod
    def held(i, c):
        core = lax.rem(i, 2)
        return lax.rem(i // 2 - c // 2 - 4 * core + 16, 8) * 2 + core

    @staticmethod
    def holder(share, c):
        core = lax.rem(share, 2)
        return lax.rem(c // 2 + share // 2 + 4 * core, 8) * 2 + core

    def col_target(self, way):
        if way == "x":
            return (((1 - self.lo) * 4 + self.y) * 2 + self.core, self.c)
        if way == "c":
            return ((self.lo * 4 + self.y) * 2 + 1 - self.core, self.c)
        step = self.sign * STEPS[way]
        return ((self.lo * 4 + lax.rem(self.y + step + 4, 4)) * 2 + self.core, self.c)


class Gather:
    def __init__(self, place, kind, tree, buf, send, recv, pieces, own):
        self.kind, self.buf, self.send, self.recv = kind, buf, send, recv
        self.pieces, self.own = pieces, own
        self.tree = tree
        self.ids = ROW_ID if kind == "row" else COL_ID
        self.share = place.row_share if kind == "row" else place.col_share
        self.target = place.row_target if kind == "row" else place.col_target
        self.depth = buf.shape[1] // pieces

    def copy(self, share, way, child, piece, source):
        rows = pl.ds(piece * self.depth, self.depth)
        n = self.ids[child]
        return pltpu.make_async_remote_copy(
            src_ref=source.at[rows],
            dst_ref=self.buf.at[share, rows],
            send_sem=self.send.at[n, piece],
            recv_sem=self.recv.at[n, piece],
            device_id=self.target(way),
            device_id_type=MESH,
        )

    def start(self, slot, piece, ways=None, source=None):
        share = self.share(slot)
        source = self.buf.at[share] if source is None else source
        for way, child in self.tree[slot]:
            if ways is None or way in ways:
                self.copy(share, way, child, piece, source).start()

    def arrive(self, slot, piece):
        rows = pl.ds(piece * self.depth, self.depth)
        part = self.buf.at[self.share(slot), rows]
        n = self.ids[slot]
        pltpu.make_async_copy(part, part, self.recv.at[n, piece]).wait()

    def drain(self):
        root = next(iter(self.tree))
        for slot, n in self.ids.items():
            if slot == root:
                continue
            for piece in range(self.pieces):
                rows = pl.ds(piece * self.depth, self.depth)
                part = self.buf.at[0, rows]
                pltpu.make_async_copy(part, part, self.send.at[n, piece]).wait()


PIECES = 2


def gather_kernel(
    left_ref, right_ref, v_ref, m_ref,
    red,
    vrow, vcol, wrow, wcol, rhs2, prow, qcol, q_ref, qmid, vmid, lhs, rhs, part, paired, got_pair, got, tpart, tsum, tpair, tgot, tall, town,
    s_p, r_p, s_q, r_q, s_vr, r_vr, s_vc, r_vc, s_wr, r_wr, s_wc, r_wc,
    s_one, r_one, s_two, r_two, s_sum, r_sum, s_t, r_t, s_all, r_all,
):
    at = Place()
    i, c = at.i, at.c
    size = m_ref.shape[0]
    tile = 256

    barrier = pltpu.get_barrier_semaphore()
    held = at.held(i, c)
    middle = (lax.rem(at.z + i // 2 + 4 * at.hi, 8) * 2 + at.hi, at.z * 2 + at.core)
    opposite = held // 2
    source = (opposite * 2 + at.hi, at.z * 2 + at.core)
    beyond = (i, opposite * 2 + at.hi)
    moves = jnp.logical_or(at.core != at.hi, lax.rem(at.z + 4 * at.hi, 8) != 0)
    stays = opposite == at.z
    owner = jnp.logical_and(i == c, held == c)

    def greet(device):
        pl.semaphore_signal(barrier, inc=1, device_id=device, device_id_type=MESH)

    @pl.when(jnp.logical_not(stays))
    def _():
        greet(beyond)

    @pl.when(moves)
    def _():
        greet(middle)
        greet(source)

    @pl.when(jnp.logical_not(owner))
    def _():
        greet((c, held))
        greet((at.holder(c, i), i))

    for way in ("++", "--", "x", "+", "-"):
        greet(at.row_target(way))
    for n in range(1, 8):
        greet((lax.rem(i + 2 * n, 16), c))
    greet(at.col_target("c"))
    for n in range(1, 16):
        j = lax.rem(c + n, 16)
        greet((at.holder(c, j), j))
        greet((lax.rem(i + n, 16), held))

    @pl.when(held != c)
    def _():
        greet((at.holder(c, c), c))
        greet((i, held))

    left, right = left_ref[...], right_ref[...]
    q_ref[...] = jnp.concatenate([-right, left], axis=0).T
    prow[c] = jnp.concatenate([left, right], axis=0).T
    vrow[c] = v_ref[...]
    red[...] = m_ref[...]

    @pl.when(jnp.logical_not(moves))
    def _():
        qmid[...] = q_ref[...]
        vmid[...] = v_ref[...]

    peers = 43 + jnp.where(held != c, 2, 0) + jnp.where(stays, 0, 1) + jnp.where(moves, 2, 0) + jnp.where(owner, 0, 2)
    pl.semaphore_wait(barrier, peers)

    @pl.when(jnp.logical_and(jnp.logical_not(moves), stays))
    def _():
        qcol[held] = q_ref[...]
        vcol[held] = v_ref[...]

    g_p = Gather(at, "row", ROW_TREE, prow, s_p, r_p, PIECES, None)
    g_q = Gather(at, "col", COL_TREE, qcol, s_q, r_q, PIECES, q_ref)
    g_vr = Gather(at, "row", ROW_FLAT, vrow, s_vr, r_vr, 1, v_ref)
    g_vc = Gather(at, "col", COL_FLAT, vcol, s_vc, r_vc, 1, v_ref)
    g_wr = Gather(at, "row", ROW_FLAT, wrow, s_wr, r_wr, 1, None)
    g_wc = Gather(at, "col", COL_FLAT, wcol, s_wc, r_wc, 1, None)

    crossings = ((g_vc, v_ref, vmid, 0, 0),) + tuple((g_q, q_ref, qmid, n, 1 + n) for n in range(PIECES))

    def first_copy(gather, own, mid, piece, n, direct):
        rows = pl.ds(piece * gather.depth, gather.depth)
        return pltpu.make_async_remote_copy(
            src_ref=own.at[rows],
            dst_ref=gather.buf.at[c, rows] if direct else mid.at[rows],
            send_sem=s_one.at[n],
            recv_sem=r_one.at[n],
            device_id=middle,
            device_id_type=MESH,
        )

    def second_copy(gather, own, mid, piece, n):
        rows = pl.ds(piece * gather.depth, gather.depth)
        return pltpu.make_async_remote_copy(
            src_ref=mid.at[rows],
            dst_ref=gather.buf.at[at.z * 2 + at.core, rows],
            send_sem=s_two.at[n],
            recv_sem=r_two.at[n],
            device_id=beyond,
            device_id_type=MESH,
        )

    g_vr.start((0, 0), 0)

    @pl.when(jnp.logical_and(moves, i // 2 == at.z))
    def _():
        for args in crossings:
            first_copy(*args, True).start()

    @pl.when(jnp.logical_and(moves, i // 2 != at.z))
    def _():
        for args in crossings:
            first_copy(*args, False).start()

    for piece in range(PIECES):
        g_p.start((0, 0), piece, ways=("+", "-"))

    def relay(gather, own, mid, piece, n):
        rows = pl.ds(piece * gather.depth, gather.depth)

        @pl.when(moves)
        def _():
            pltpu.make_async_copy(mid.at[rows], mid.at[rows], r_one.at[n]).wait()

        @pl.when(jnp.logical_not(stays))
        def _():
            second_copy(gather, own, mid, piece, n).start()

    def crossed(gather, own, mid, piece, n):
        rows = pl.ds(piece * gather.depth, gather.depth)

        @pl.when(jnp.logical_not(stays))
        def _():
            part = gather.buf.at[held, rows]
            pltpu.make_async_copy(part, part, r_two.at[n]).wait()

        gather.start((0, 0, 0), piece)

    def row_step(gather, slot):
        for piece in range(gather.pieces):
            gather.arrive(slot, piece)
            gather.start(slot, piece)

    def col_step(gather, slot):
        for piece in range(gather.pieces):
            gather.arrive(slot, piece)
            gather.start(slot, piece)

    def accumulate(first, second):
        k1, k2 = at.row_share(first), at.row_share(second)
        for n, k in enumerate((k1, k2)):
            high, low = halves(prow[k])
            lhs[:, pl.ds(n * 128, 128)] = high
            lhs[:, pl.ds(256 + n * 128, 128)] = low
            lhs[:, pl.ds(512 + n * 128, 128)] = high
            high, low = halves(qcol[k])
            rhs[:, pl.ds(n * 128, 128)] = high
            rhs[:, pl.ds(256 + n * 128, 128)] = high
            rhs[:, pl.ds(512 + n * 128, 128)] = low

        for t in range(size // tile):
            band = pl.ds(t * tile, tile)
            red[band, :] += dot(lhs[band, :], rhs[...], NT)

    def run(step, gather, *slots):
        for slot in slots:
            step(gather, slot)

    width = v_ref.shape[0]
    count = 16 * width
    sibling = at.col_target("c")

    def factor():
        vh, vl = halves(vrow[...].reshape(count, size))
        ph, pl_ = halves(prow[c])
        tpart[...] = (dot(vh, ph, NN) + dot(vh, pl_, NN) + dot(vl, ph, NN)).reshape(8, 2, width, 128)
        tpaired().start()

    def image_first():
        vh, vl = halves(vrow[...].reshape(count, size))
        high, low = halves(m_ref[...])
        lhs[...] = high
        rhs[...] = low
        part[...] = (
            dot(vh, lhs[...], NN) + dot(vh, rhs[...], NN) + dot(vl, lhs[...], NN)
        ).reshape(8, 2, width, size)

    def tpaired():
        return pltpu.make_async_remote_copy(
            src_ref=tpart.at[:, 1 - at.core],
            dst_ref=tpair,
            send_sem=s_t.at[7],
            recv_sem=r_t.at[7],
            device_id=sibling,
            device_id_type=MESH,
        )

    def taddend(n):
        other = lax.rem(i + 2 * n, 16)
        return pltpu.make_async_remote_copy(
            src_ref=tsum.at[other // 2],
            dst_ref=tgot.at[n - 1],
            send_sem=s_t.at[n - 1],
            recv_sem=r_t.at[n - 1],
            device_id=(other, c),
            device_id_type=MESH,
        )

    def factor_sums():
        tpaired().wait_recv()
        tsum[...] = tpart[:, at.core] + tpair[...]
        for n in (2, 6, 1, 3, 5, 7, 4):
            taddend(n).start()

    def tspread(n):
        j = lax.rem(c + n, 16)
        return pltpu.make_async_remote_copy(
            src_ref=town,
            dst_ref=tall.at[i],
            send_sem=s_all.at[n],
            recv_sem=r_all.at[i],
            device_id=(at.holder(c, j), j),
            device_id_type=MESH,
        )

    def factor_spread():
        total = tsum[i // 2]
        for n in (1, 3, 5, 7, 4, 2, 6):
            taddend(n).wait_recv()
            total += tgot[n - 1]
        town[...] = total

        @pl.when(held != c)
        def _():
            tspread(0).start()

        @pl.when(held == c)
        def _():
            tall[i] = town[...]

        for n in (8, 7, 9, 6, 10, 5, 11, 4, 12, 3, 13, 2, 14, 1, 15):
            tspread(n).start()

    def from_row(n):
        row = lax.rem(i + n, 16)
        pltpu.make_async_copy(tall.at[row], tall.at[row], r_all.at[row]).wait()

    def image():
        for n in range(1, 16):
            from_row(n)

        @pl.when(held != c)
        def _():
            from_row(0)

        th, tl = halves(tall[...].reshape(count, 128))
        qh, ql = halves(qcol[held])
        more = dot(th, qh, NT) + dot(th, ql, NT) + dot(tl, qh, NT)
        part[...] = -(part[...] + more.reshape(8, 2, width, size))
        paired_copy().start()

    def paired_copy():
        return pltpu.make_async_remote_copy(
            src_ref=part.at[:, 1 - at.core],
            dst_ref=got_pair,
            send_sem=s_sum.at[7],
            recv_sem=r_sum.at[7],
            device_id=sibling,
            device_id_type=MESH,
        )

    def addend(n):
        other = lax.rem(i + 2 * n, 16)
        return pltpu.make_async_remote_copy(
            src_ref=paired.at[at.held(other, c) // 2],
            dst_ref=got.at[n - 1],
            send_sem=s_sum.at[n - 1],
            recv_sem=r_sum.at[n - 1],
            device_id=(other, c),
            device_id_type=MESH,
        )

    def image_sums():
        paired_copy().wait_recv()
        paired[...] = part[:, at.core] + got_pair[...]
        for n in (2, 6, 1, 3, 5, 7, 4):
            addend(n).start()

    last = 1 + PIECES

    def home():
        return pltpu.make_async_remote_copy(
            src_ref=wcol.at[held],
            dst_ref=wrow.at[held],
            send_sem=s_one.at[last],
            recv_sem=r_one.at[last],
            device_id=(c, held),
            device_id_type=MESH,
        )

    def image_share():
        total = paired[opposite]
        for n in (1, 3, 5, 7, 4, 2, 6):
            addend(n).wait_recv()
            total += got[n - 1]
        wcol[held] = total

        @pl.when(jnp.logical_not(owner))
        def _():
            home().start()

        @pl.when(owner)
        def _():
            wrow[c] = wcol[held]

        g_wc.start((0, 0, 0), 0)

    def image_home():
        @pl.when(jnp.logical_not(owner))
        def _():
            home().wait_recv()

        g_wr.start((0, 0), 0)

    def stage(target, flat):
        high, low = halves(flat)
        target[:count] = high
        target[count : 2 * count] = high
        target[2 * count :] = low

    def outer(rows_ref, right):
        high, low = halves(rows_ref[...].reshape(count, size).T)
        lhs[:, :count] = high
        lhs[:, count : 2 * count] = low
        lhs[:, 2 * count :] = high
        for t in range(size // tile):
            band = pl.ds(t * tile, tile)
            red[band, :] += dot(lhs[band, :], right[...], NN)

    def first_outer():
        stage(rhs, wcol[...].reshape(count, size))
        outer(vrow, rhs)
        stage(rhs2, -vcol[...].reshape(count, size))

    def last_outer():
        outer(wrow, rhs2)

    for args in crossings[:1]:
        relay(*args)
    run(row_step, g_vr, (2, 0), (-2, 0), (1, 0), (-1, 0))
    for args in crossings[1:]:
        relay(*args)
    run(row_step, g_p, (1, 0), (-1, 0))
    run(row_step, g_vr, (3, 0), (-3, 0), (4, 0))
    for piece in range(PIECES):
        g_p.start((0, 0), piece, ways=("x",))
    run(row_step, g_vr, (0, 1), (1, 1), (-1, 1), (2, 1), (-2, 1), (3, 1), (-3, 1), (4, 1))
    factor()
    factor_sums()
    for args in crossings:
        crossed(*args)
    factor_spread()
    run(row_step, g_p, (2, 0), (-2, 0))
    run(row_step, g_p, (0, 1))
    image_first()
    run(col_step, g_q, (1, 0, 0), (-1, 0, 0), (0, 1, 0))
    image()
    image_sums()
    run(row_step, g_p, (3, 0), (-3, 0))
    run(col_step, g_vc, (1, 0, 0), (-1, 0, 0), (2, 0, 0), (0, 1, 0))
    run(col_step, g_q, (1, 1, 0), (-1, 1, 0), (2, 0, 0), *COL_SLOTS[8:15])
    run(row_step, g_p, (1, 1), (-1, 1))

    late = (at.col_share((2, 1, 0)), at.col_share((2, 1, 1)))
    pairs = (((0, 0), (0, 1)), ((1, 0), (-1, 0)), ((2, 0), (-2, 0)), ((3, 0), (-3, 0)), ((1, 1), (-1, 1)))

    def ready(n):
        is_ready = None
        for slot in pairs[n]:
            for share in late:
                test = at.row_share(slot) != share
                is_ready = test if is_ready is None else jnp.logical_and(is_ready, test)
        return is_ready

    def early(*numbers):
        for n in numbers:

            @pl.when(ready(n))
            def _():
                accumulate(*pairs[n])

    def remaining():
        for n in range(len(pairs)):

            @pl.when(jnp.logical_not(ready(n)))
            def _():
                accumulate(*pairs[n])

    early(0)
    run(row_step, g_p, (2, 1))
    early(1)
    run(row_step, g_p, (-2, 1))
    early(2)
    run(row_step, g_p, (4, 0))
    early(3)
    image_share()
    early(4)
    run(col_step, g_q, (2, 1, 0), (2, 1, 1))
    remaining()
    run(col_step, g_wc, (1, 0, 0), (-1, 0, 0), (2, 0, 0))
    image_home()
    accumulate((2, 1), (-2, 1))
    run(row_step, g_wr, (1, 0), (-1, 0), (2, 0), (-2, 0))
    run(row_step, g_p, (3, 1), (-3, 1))
    accumulate((3, 1), (-3, 1))
    run(row_step, g_wr, (3, 0), (-3, 0), (4, 0))
    run(row_step, g_p, (4, 1))
    run(col_step, g_vc, (1, 1, 0), (-1, 1, 0), (2, 1, 0))
    run(col_step, g_wc, (0, 1, 0), (1, 1, 0), (-1, 1, 0), (2, 1, 0))
    accumulate((4, 0), (4, 1))
    run(col_step, g_vc, *COL_SLOTS[8:])
    run(col_step, g_wc, *COL_SLOTS[8:])
    first_outer()
    run(row_step, g_wr, (0, 1), (1, 1), (-1, 1), (2, 1), (-2, 1), (3, 1), (-3, 1), (4, 1))
    last_outer()

    for gather in (g_p, g_q, g_vr, g_vc, g_wr, g_wc):
        gather.drain()

    @pl.when(moves)
    def _():
        for gather, own, mid, piece, n in crossings:
            part = own.at[pl.ds(piece * gather.depth, gather.depth)]
            pltpu.make_async_copy(part, part, s_one.at[n]).wait()

    @pl.when(jnp.logical_not(stays))
    def _():
        for gather, own, mid, piece, n in crossings:
            part = mid.at[pl.ds(piece * gather.depth, gather.depth)]
            pltpu.make_async_copy(part, part, s_two.at[n]).wait()

    @pl.when(jnp.logical_not(owner))
    def _():
        home().wait_send()

    @pl.when(held != c)
    def _():
        tspread(0).wait_send()

    for n in range(1, 16):
        tspread(n).wait_send()
    for n in range(1, 8):
        addend(n).wait_send()
        taddend(n).wait_send()
    paired_copy().wait_send()
    tpaired().wait_send()


def copy_kernel(source, out):
    out[...] = source[...]


def local(matrix, left_panel, right_panel, reflectors):
    size = matrix.shape[0]
    width = reflectors.shape[1]
    vmem = pl.BlockSpec(memory_space=pltpu.VMEM)
    dma = pltpu.SemaphoreType.DMA
    sems = [dma((16, PIECES))] * 4 + [dma((16, 1))] * 8 + [dma((2 + PIECES,))] * 4 + [dma((8,))] * 4 + [dma((16,))] * 2
    block = pl.BlockSpec((size // 4, size), lambda n: (n, 0))
    updated = pl.pallas_call(
        gather_kernel,
        name="gather",
        out_shape=jax.ShapeDtypeStruct((size, size), F32),
        in_specs=[vmem] * 4,
        out_specs=vmem,
        scratch_shapes=[pltpu.VMEM((16, width, size), F32)] * 4
        + [
            pltpu.VMEM((size, size), BF16),
            pltpu.VMEM((16, size, 128), F32),
            pltpu.VMEM((16, size, 128), F32),
            pltpu.VMEM((size, 128), F32),
            pltpu.VMEM((size, 128), F32),
            pltpu.VMEM((width, size), F32),
            pltpu.VMEM((size, size), BF16),
            pltpu.VMEM((size, size), BF16),
            pltpu.VMEM((8, 2, width, size), F32),
            pltpu.VMEM((8, width, size), F32),
            pltpu.VMEM((8, width, size), F32),
            pltpu.VMEM((7, width, size), F32),
            pltpu.VMEM((8, 2, width, 128), F32),
            pltpu.VMEM((8, width, 128), F32),
            pltpu.VMEM((8, width, 128), F32),
            pltpu.VMEM((7, width, 128), F32),
            pltpu.VMEM((16, width, 128), F32),
            pltpu.VMEM((width, 128), F32),
        ]
        + sems,
        compiler_params=pltpu.CompilerParams(
            collective_id=0, has_side_effects=True, vmem_limit_bytes=56 * 1024 * 1024
        ),
    )(left_panel.T, right_panel.T, reflectors.T, matrix)
    return pl.pallas_call(
        copy_kernel,
        name="hand_over",
        grid=(4,),
        out_shape=jax.ShapeDtypeStruct((size, size), F32),
        in_specs=[block],
        out_specs=block,
    )(updated)


def solution(mesh):
    in_specs = (P("row", "col"), P("row", "col"), P("row", "col"), P("row", "col"))
    out_specs = P("row", "col")
    return jax.shard_map(local, mesh=mesh, in_specs=in_specs, out_specs=out_specs, check_vma=False)
```

```python
import functools

import jax
import jax.numpy as jnp
from jax import lax
from jax.experimental import pallas as pl
from jax.experimental.pallas import tpu as pltpu
from jax.sharding import PartitionSpec as P

F32 = jnp.float32
BF16 = jnp.bfloat16
MESH = pl.DeviceIdType.MESH

ROW_TREE = {
    (0, 0): (("+", (1, 0)), ("-", (-1, 0)), ("x", (0, 1))),
    (1, 0): (("+", (2, 0)),),
    (-1, 0): (("-", (-2, 0)),),
    (0, 1): (("+", (1, 1)), ("-", (-1, 1))),
    (2, 0): (("+", (3, 0)), ("x", (2, 1))),
    (-2, 0): (("-", (-3, 0)), ("x", (-2, 1))),
    (3, 0): (("+", (4, 0)),),
    (-3, 0): (),
    (1, 1): (),
    (-1, 1): (),
    (2, 1): (("+", (3, 1)),),
    (-2, 1): (("-", (-3, 1)),),
    (4, 0): (("x", (4, 1)),),
    (3, 1): (),
    (-3, 1): (),
    (4, 1): (),
}
COL_TREE = {
    (0, 0, 0): (("x", (0, 1, 0)), ("+", (1, 0, 0)), ("-", (-1, 0, 0)), ("c", (0, 0, 1))),
    (1, 0, 0): (("+", (2, 0, 0)), ("c", (1, 0, 1))),
    (-1, 0, 0): (("c", (-1, 0, 1)),),
    (0, 1, 0): (("+", (1, 1, 0)), ("-", (-1, 1, 0)), ("c", (0, 1, 1))),
    (2, 0, 0): (("c", (2, 0, 1)),),
    (1, 1, 0): (("+", (2, 1, 0)), ("c", (1, 1, 1))),
    (-1, 1, 0): (("c", (-1, 1, 1)),),
    (2, 1, 0): (("c", (2, 1, 1)),),
    (0, 0, 1): (),
    (1, 0, 1): (),
    (-1, 0, 1): (),
    (0, 1, 1): (),
    (2, 0, 1): (),
    (1, 1, 1): (),
    (-1, 1, 1): (),
    (2, 1, 1): (),
}
ROW_FLAT = {
    (0, 0): (("++", (2, 0)), ("--", (-2, 0)), ("+", (1, 0)), ("-", (-1, 0)), ("x", (0, 1))),
    (1, 0): (("x", (1, 1)),),
    (-1, 0): (("x", (-1, 1)),),
    (0, 1): (),
    (2, 0): (("++", (4, 0)), ("+", (3, 0)), ("x", (2, 1))),
    (-2, 0): (("-", (-3, 0)), ("x", (-2, 1))),
    (3, 0): (("x", (3, 1)),),
    (-3, 0): (("x", (-3, 1)),),
    (1, 1): (),
    (-1, 1): (),
    (2, 1): (),
    (-2, 1): (),
    (4, 0): (("x", (4, 1)),),
    (3, 1): (),
    (-3, 1): (),
    (4, 1): (),
}
COL_FLAT = {
    (0, 0, 0): (("++", (2, 0, 0)), ("+", (1, 0, 0)), ("-", (-1, 0, 0)), ("x", (0, 1, 0)), ("c", (0, 0, 1))),
    (1, 0, 0): (("x", (1, 1, 0)), ("c", (1, 0, 1))),
    (-1, 0, 0): (("x", (-1, 1, 0)), ("c", (-1, 0, 1))),
    (0, 1, 0): (("c", (0, 1, 1)),),
    (2, 0, 0): (("x", (2, 1, 0)), ("c", (2, 0, 1))),
    (1, 1, 0): (("c", (1, 1, 1)),),
    (-1, 1, 0): (("c", (-1, 1, 1)),),
    (2, 1, 0): (("c", (2, 1, 1)),),
    (0, 0, 1): (),
    (1, 0, 1): (),
    (-1, 0, 1): (),
    (0, 1, 1): (),
    (2, 0, 1): (),
    (1, 1, 1): (),
    (-1, 1, 1): (),
    (2, 1, 1): (),
}
STEPS = {"+": 1, "-": -1, "++": 2, "--": -2}
ROW_SLOTS = tuple(ROW_TREE)
COL_SLOTS = tuple(COL_TREE)
ROW_ID = {slot: n for n, slot in enumerate(ROW_SLOTS)}
COL_ID = {slot: n for n, slot in enumerate(COL_SLOTS)}


def halves(x):
    high = x.astype(BF16)
    return high, (x - high.astype(F32)).astype(BF16)


def dot(a, b, dims):
    return lax.dot_general(a, b, (dims, ((), ())), preferred_element_type=F32)


NT = ((1,), (1,))
NN = ((1,), (0,))


class Place:
    def __init__(self):
        self.i = lax.axis_index("row")
        self.c = lax.axis_index("col")
        self.core = lax.rem(self.i, 2)
        self.y = lax.rem(self.i // 2, 4)
        self.lo = self.i // 8
        self.z = self.c // 2
        self.hi = lax.rem(self.c, 2)
        self.sign = 1 - 2 * self.core

    def row_share(self, slot):
        d, l = slot
        z = lax.rem(self.z - self.sign * d + 8, 8)
        hi = self.hi if l == 0 else 1 - self.hi
        return z * 2 + hi

    def row_target(self, way):
        if way == "x":
            return (self.i, self.z * 2 + 1 - self.hi)
        step = self.sign * STEPS[way]
        return (self.i, lax.rem(self.z + step + 8, 8) * 2 + self.hi)

    def col_share(self, slot):
        d, l, s = slot
        sign = self.sign if s == 0 else -self.sign
        y = lax.rem(self.y - sign * d + 4, 4)
        lo = self.lo if l == 0 else 1 - self.lo
        core = self.core if s == 0 else 1 - self.core
        return self.held((lo * 4 + y) * 2 + core, self.c)

    @staticmethod
    def held(i, c):
        core = lax.rem(i, 2)
        return lax.rem(i // 2 - c // 2 - 4 * core + 16, 8) * 2 + core

    @staticmethod
    def holder(share, c):
        core = lax.rem(share, 2)
        return lax.rem(c // 2 + share // 2 + 4 * core, 8) * 2 + core

    def col_target(self, way):
        if way == "x":
            return (((1 - self.lo) * 4 + self.y) * 2 + self.core, self.c)
        if way == "c":
            return ((self.lo * 4 + self.y) * 2 + 1 - self.core, self.c)
        step = self.sign * STEPS[way]
        return ((self.lo * 4 + lax.rem(self.y + step + 4, 4)) * 2 + self.core, self.c)


class Gather:
    def __init__(self, place, kind, tree, buf, send, recv, pieces, own):
        self.kind, self.buf, self.send, self.recv = kind, buf, send, recv
        self.pieces, self.own = pieces, own
        self.tree = tree
        self.ids = ROW_ID if kind == "row" else COL_ID
        self.share = place.row_share if kind == "row" else place.col_share
        self.target = place.row_target if kind == "row" else place.col_target
        self.depth = buf.shape[1] // pieces

    def copy(self, share, way, child, piece, source):
        rows = pl.ds(piece * self.depth, self.depth)
        n = self.ids[child]
        return pltpu.make_async_remote_copy(
            src_ref=source.at[rows],
            dst_ref=self.buf.at[share, rows],
            send_sem=self.send.at[n, piece],
            recv_sem=self.recv.at[n, piece],
            device_id=self.target(way),
            device_id_type=MESH,
        )

    def start(self, slot, piece, ways=None, source=None):
        share = self.share(slot)
        source = self.buf.at[share] if source is None else source
        for way, child in self.tree[slot]:
            if ways is None or way in ways:
                self.copy(share, way, child, piece, source).start()

    def arrive(self, slot, piece):
        rows = pl.ds(piece * self.depth, self.depth)
        part = self.buf.at[self.share(slot), rows]
        n = self.ids[slot]
        pltpu.make_async_copy(part, part, self.recv.at[n, piece]).wait()

    def drain(self):
        root = next(iter(self.tree))
        for slot, n in self.ids.items():
            if slot == root:
                continue
            for piece in range(self.pieces):
                rows = pl.ds(piece * self.depth, self.depth)
                part = self.buf.at[0, rows]
                pltpu.make_async_copy(part, part, self.send.at[n, piece]).wait()


PIECES = 2


def gather_kernel(
    left_ref, right_ref, v_ref, m_ref,
    red,
    vrow, vcol, wrow, wcol, rhs2, prow, qcol, q_ref, qmid, vmid, lhs, rhs, part, paired, got_pair, got, tpart, tsum, tpair, tgot, tall, town,
    s_p, r_p, s_q, r_q, s_vr, r_vr, s_vc, r_vc, s_wr, r_wr, s_wc, r_wc,
    s_one, r_one, s_two, r_two, s_sum, r_sum, s_t, r_t, s_all, r_all,
):
    at = Place()
    i, c = at.i, at.c
    size = m_ref.shape[0]
    tile = 256

    barrier = pltpu.get_barrier_semaphore()
    held = at.held(i, c)
    middle = (lax.rem(at.z + i // 2 + 4 * at.hi, 8) * 2 + at.hi, at.z * 2 + at.core)
    opposite = held // 2
    source = (opposite * 2 + at.hi, at.z * 2 + at.core)
    beyond = (i, opposite * 2 + at.hi)
    moves = jnp.logical_or(at.core != at.hi, lax.rem(at.z + 4 * at.hi, 8) != 0)
    stays = opposite == at.z
    owner = jnp.logical_and(i == c, held == c)

    def greet(device):
        pl.semaphore_signal(barrier, inc=1, device_id=device, device_id_type=MESH)

    @pl.when(jnp.logical_not(stays))
    def _():
        greet(beyond)

    @pl.when(moves)
    def _():
        greet(middle)
        greet(source)

    @pl.when(jnp.logical_not(owner))
    def _():
        greet((c, held))
        greet((at.holder(c, i), i))

    for way in ("++", "--", "x", "+", "-"):
        greet(at.row_target(way))
    for n in range(1, 8):
        greet((lax.rem(i + 2 * n, 16), c))
    greet(at.col_target("c"))
    for n in range(1, 16):
        j = lax.rem(c + n, 16)
        greet((at.holder(c, j), j))
        greet((lax.rem(i + n, 16), held))

    @pl.when(held != c)
    def _():
        greet((at.holder(c, c), c))
        greet((i, held))

    left, right = left_ref[...], right_ref[...]
    q_ref[...] = jnp.concatenate([-right, left], axis=0).T
    prow[c] = jnp.concatenate([left, right], axis=0).T
    vrow[c] = v_ref[...]
    red[...] = m_ref[...]

    @pl.when(jnp.logical_not(moves))
    def _():
        qmid[...] = q_ref[...]
        vmid[...] = v_ref[...]

    peers = 43 + jnp.where(held != c, 2, 0) + jnp.where(stays, 0, 1) + jnp.where(moves, 2, 0) + jnp.where(owner, 0, 2)
    pl.semaphore_wait(barrier, peers)

    @pl.when(jnp.logical_and(jnp.logical_not(moves), stays))
    def _():
        qcol[held] = q_ref[...]
        vcol[held] = v_ref[...]

    g_p = Gather(at, "row", ROW_TREE, prow, s_p, r_p, PIECES, None)
    g_q = Gather(at, "col", COL_TREE, qcol, s_q, r_q, PIECES, q_ref)
    g_vr = Gather(at, "row", ROW_FLAT, vrow, s_vr, r_vr, 1, v_ref)
    g_vc = Gather(at, "col", COL_FLAT, vcol, s_vc, r_vc, 1, v_ref)
    g_wr = Gather(at, "row", ROW_FLAT, wrow, s_wr, r_wr, 1, None)
    g_wc = Gather(at, "col", COL_FLAT, wcol, s_wc, r_wc, 1, None)

    crossings = ((g_vc, v_ref, vmid, 0, 0),) + tuple((g_q, q_ref, qmid, n, 1 + n) for n in range(PIECES))

    def first_copy(gather, own, mid, piece, n, direct):
        rows = pl.ds(piece * gather.depth, gather.depth)
        return pltpu.make_async_remote_copy(
            src_ref=own.at[rows],
            dst_ref=gather.buf.at[c, rows] if direct else mid.at[rows],
            send_sem=s_one.at[n],
            recv_sem=r_one.at[n],
            device_id=middle,
            device_id_type=MESH,
        )

    def second_copy(gather, own, mid, piece, n):
        rows = pl.ds(piece * gather.depth, gather.depth)
        return pltpu.make_async_remote_copy(
            src_ref=mid.at[rows],
            dst_ref=gather.buf.at[at.z * 2 + at.core, rows],
            send_sem=s_two.at[n],
            recv_sem=r_two.at[n],
            device_id=beyond,
            device_id_type=MESH,
        )

    g_vr.start((0, 0), 0)

    @pl.when(jnp.logical_and(moves, i // 2 == at.z))
    def _():
        for args in crossings:
            first_copy(*args, True).start()

    @pl.when(jnp.logical_and(moves, i // 2 != at.z))
    def _():
        for args in crossings:
            first_copy(*args, False).start()

    for piece in range(PIECES):
        g_p.start((0, 0), piece, ways=("+", "-"))

    def relay(gather, own, mid, piece, n):
        rows = pl.ds(piece * gather.depth, gather.depth)

        @pl.when(moves)
        def _():
            pltpu.make_async_copy(mid.at[rows], mid.at[rows], r_one.at[n]).wait()

        @pl.when(jnp.logical_not(stays))
        def _():
            second_copy(gather, own, mid, piece, n).start()

    def crossed(gather, own, mid, piece, n):
        rows = pl.ds(piece * gather.depth, gather.depth)

        @pl.when(jnp.logical_not(stays))
        def _():
            part = gather.buf.at[held, rows]
            pltpu.make_async_copy(part, part, r_two.at[n]).wait()

        gather.start((0, 0, 0), piece)

    def row_step(gather, slot):
        for piece in range(gather.pieces):
            gather.arrive(slot, piece)
            gather.start(slot, piece)

    def col_step(gather, slot):
        for piece in range(gather.pieces):
            gather.arrive(slot, piece)
            gather.start(slot, piece)

    def accumulate(first, second):
        k1, k2 = at.row_share(first), at.row_share(second)
        for n, k in enumerate((k1, k2)):
            high, low = halves(prow[k])
            lhs[:, pl.ds(n * 128, 128)] = high
            lhs[:, pl.ds(256 + n * 128, 128)] = low
            lhs[:, pl.ds(512 + n * 128, 128)] = high
            high, low = halves(qcol[k])
            rhs[:, pl.ds(n * 128, 128)] = high
            rhs[:, pl.ds(256 + n * 128, 128)] = high
            rhs[:, pl.ds(512 + n * 128, 128)] = low

        for t in range(size // tile):
            band = pl.ds(t * tile, tile)
            red[band, :] += dot(lhs[band, :], rhs[...], NT)

    def run(step, gather, *slots):
        for slot in slots:
            step(gather, slot)

    width = v_ref.shape[0]
    count = 16 * width
    sibling = at.col_target("c")

    def factor():
        vh, vl = halves(vrow[...].reshape(count, size))
        ph, pl_ = halves(prow[c])
        tpart[...] = (dot(vh, ph, NN) + dot(vh, pl_, NN) + dot(vl, ph, NN)).reshape(8, 2, width, 128)
        tpaired().start()

    def image_first():
        vh, vl = halves(vrow[...].reshape(count, size))
        high, low = halves(m_ref[...])
        lhs[...] = high
        rhs[...] = low
        part[...] = (
            dot(vh, lhs[...], NN) + dot(vh, rhs[...], NN) + dot(vl, lhs[...], NN)
        ).reshape(8, 2, width, size)

    def tpaired():
        return pltpu.make_async_remote_copy(
            src_ref=tpart.at[:, 1 - at.core],
            dst_ref=tpair,
            send_sem=s_t.at[7],
            recv_sem=r_t.at[7],
            device_id=sibling,
            device_id_type=MESH,
        )

    def taddend(n):
        other = lax.rem(i + 2 * n, 16)
        return pltpu.make_async_remote_copy(
            src_ref=tsum.at[other // 2],
            dst_ref=tgot.at[n - 1],
            send_sem=s_t.at[n - 1],
            recv_sem=r_t.at[n - 1],
            device_id=(other, c),
            device_id_type=MESH,
        )

    def factor_sums():
        tpaired().wait_recv()
        tsum[...] = tpart[:, at.core] + tpair[...]
        for n in (2, 6, 1, 3, 5, 7, 4):
            taddend(n).start()

    def tspread(n):
        j = lax.rem(c + n, 16)
        return pltpu.make_async_remote_copy(
            src_ref=town,
            dst_ref=tall.at[i],
            send_sem=s_all.at[n],
            recv_sem=r_all.at[i],
            device_id=(at.holder(c, j), j),
            device_id_type=MESH,
        )

    def factor_spread():
        total = tsum[i // 2]
        for n in (1, 3, 5, 7, 4, 2, 6):
            taddend(n).wait_recv()
            total += tgot[n - 1]
        town[...] = total

        @pl.when(held != c)
        def _():
            tspread(0).start()

        @pl.when(held == c)
        def _():
            tall[i] = town[...]

        for n in (8, 7, 9, 6, 10, 5, 11, 4, 12, 3, 13, 2, 14, 1, 15):
            tspread(n).start()

    def from_row(n):
        row = lax.rem(i + n, 16)
        pltpu.make_async_copy(tall.at[row], tall.at[row], r_all.at[row]).wait()

    def image():
        for n in range(1, 16):
            from_row(n)

        @pl.when(held != c)
        def _():
            from_row(0)

        th, tl = halves(tall[...].reshape(count, 128))
        qh, ql = halves(qcol[held])
        more = dot(th, qh, NT) + dot(th, ql, NT) + dot(tl, qh, NT)
        part[...] = -(part[...] + more.reshape(8, 2, width, size))
        paired_copy().start()

    def paired_copy():
        return pltpu.make_async_remote_copy(
            src_ref=part.at[:, 1 - at.core],
            dst_ref=got_pair,
            send_sem=s_sum.at[7],
            recv_sem=r_sum.at[7],
            device_id=sibling,
            device_id_type=MESH,
        )

    def addend(n):
        other = lax.rem(i + 2 * n, 16)
        return pltpu.make_async_remote_copy(
            src_ref=paired.at[at.held(other, c) // 2],
            dst_ref=got.at[n - 1],
            send_sem=s_sum.at[n - 1],
            recv_sem=r_sum.at[n - 1],
            device_id=(other, c),
            device_id_type=MESH,
        )

    def image_sums():
        paired_copy().wait_recv()
        paired[...] = part[:, at.core] + got_pair[...]
        for n in (2, 6, 1, 3, 5, 7, 4):
            addend(n).start()

    last = 1 + PIECES

    def home():
        return pltpu.make_async_remote_copy(
            src_ref=wcol.at[held],
            dst_ref=wrow.at[held],
            send_sem=s_one.at[last],
            recv_sem=r_one.at[last],
            device_id=(c, held),
            device_id_type=MESH,
        )

    def image_share():
        total = paired[opposite]
        for n in (1, 3, 5, 7, 4, 2, 6):
            addend(n).wait_recv()
            total += got[n - 1]
        wcol[held] = total

        @pl.when(jnp.logical_not(owner))
        def _():
            home().start()

        @pl.when(owner)
        def _():
            wrow[c] = wcol[held]

        g_wc.start((0, 0, 0), 0)

    def image_home():
        @pl.when(jnp.logical_not(owner))
        def _():
            home().wait_recv()

        g_wr.start((0, 0), 0)

    def stage(target, flat):
        high, low = halves(flat)
        target[:count] = high
        target[count : 2 * count] = high
        target[2 * count :] = low

    def outer(rows_ref, right):
        high, low = halves(rows_ref[...].reshape(count, size).T)
        lhs[:, :count] = high
        lhs[:, count : 2 * count] = low
        lhs[:, 2 * count :] = high
        for t in range(size // tile):
            band = pl.ds(t * tile, tile)
            red[band, :] += dot(lhs[band, :], right[...], NN)

    def first_outer():
        stage(rhs, wcol[...].reshape(count, size))
        outer(vrow, rhs)
        stage(rhs2, -vcol[...].reshape(count, size))

    def last_outer():
        outer(wrow, rhs2)

    for args in crossings[:1]:
        relay(*args)
    run(row_step, g_vr, (2, 0), (-2, 0), (1, 0), (-1, 0))
    for args in crossings[1:]:
        relay(*args)
    run(row_step, g_p, (1, 0), (-1, 0))
    run(row_step, g_vr, (3, 0), (-3, 0), (4, 0))
    for piece in range(PIECES):
        g_p.start((0, 0), piece, ways=("x",))
    run(row_step, g_vr, (0, 1), (1, 1), (-1, 1), (2, 1), (-2, 1), (3, 1), (-3, 1), (4, 1))
    factor()
    factor_sums()
    for args in crossings:
        crossed(*args)
    factor_spread()
    run(row_step, g_p, (2, 0), (-2, 0))
    run(row_step, g_p, (0, 1))
    image_first()
    run(col_step, g_q, (1, 0, 0), (-1, 0, 0), (0, 1, 0))
    image()
    image_sums()
    run(row_step, g_p, (3, 0), (-3, 0))
    run(col_step, g_vc, (1, 0, 0), (-1, 0, 0), (2, 0, 0), (0, 1, 0))
    run(col_step, g_q, (1, 1, 0), (-1, 1, 0), (2, 0, 0), *COL_SLOTS[8:15])
    run(row_step, g_p, (1, 1), (-1, 1))

    late = (at.col_share((2, 1, 0)), at.col_share((2, 1, 1)))
    pairs = (((0, 0), (0, 1)), ((1, 0), (-1, 0)), ((2, 0), (-2, 0)), ((3, 0), (-3, 0)), ((1, 1), (-1, 1)))

    def ready(n):
        is_ready = None
        for slot in pairs[n]:
            for share in late:
                test = at.row_share(slot) != share
                is_ready = test if is_ready is None else jnp.logical_and(is_ready, test)
        return is_ready

    def early(*numbers):
        for n in numbers:

            @pl.when(ready(n))
            def _():
                accumulate(*pairs[n])

    def remaining():
        for n in range(len(pairs)):

            @pl.when(jnp.logical_not(ready(n)))
            def _():
                accumulate(*pairs[n])

    early(0)
    run(row_step, g_p, (2, 1))
    early(1)
    run(row_step, g_p, (-2, 1))
    early(2)
    run(row_step, g_p, (4, 0))
    early(3)
    image_share()
    early(4)
    run(col_step, g_q, (2, 1, 0), (2, 1, 1))
    remaining()
    run(col_step, g_wc, (1, 0, 0), (-1, 0, 0), (2, 0, 0))
    image_home()
    accumulate((2, 1), (-2, 1))
    run(row_step, g_wr, (1, 0), (-1, 0), (2, 0), (-2, 0))
    run(row_step, g_p, (3, 1), (-3, 1))
    accumulate((3, 1), (-3, 1))
    run(row_step, g_wr, (3, 0), (-3, 0), (4, 0))
    run(row_step, g_p, (4, 1))
    run(col_step, g_vc, (1, 1, 0), (-1, 1, 0), (2, 1, 0))
    run(col_step, g_wc, (0, 1, 0), (1, 1, 0), (-1, 1, 0), (2, 1, 0))
    accumulate((4, 0), (4, 1))
    run(col_step, g_vc, *COL_SLOTS[8:])
    run(col_step, g_wc, *COL_SLOTS[8:])
    first_outer()
    run(row_step, g_wr, (0, 1), (1, 1), (-1, 1), (2, 1), (-2, 1), (3, 1), (-3, 1), (4, 1))
    last_outer()

    for gather in (g_p, g_q, g_vr, g_vc, g_wr, g_wc):
        gather.drain()

    @pl.when(moves)
    def _():
        for gather, own, mid, piece, n in crossings:
            part = own.at[pl.ds(piece * gather.depth, gather.depth)]
            pltpu.make_async_copy(part, part, s_one.at[n]).wait()

    @pl.when(jnp.logical_not(stays))
    def _():
        for gather, own, mid, piece, n in crossings:
            part = mid.at[pl.ds(piece * gather.depth, gather.depth)]
            pltpu.make_async_copy(part, part, s_two.at[n]).wait()

    @pl.when(jnp.logical_not(owner))
    def _():
        home().wait_send()

    @pl.when(held != c)
    def _():
        tspread(0).wait_send()

    for n in range(1, 16):
        tspread(n).wait_send()
    for n in range(1, 8):
        addend(n).wait_send()
        taddend(n).wait_send()
    paired_copy().wait_send()
    tpaired().wait_send()


def local(matrix, left_panel, right_panel, reflectors):
    size = matrix.shape[0]
    width = reflectors.shape[1]
    vmem = pl.BlockSpec(memory_space=pltpu.VMEM)
    dma = pltpu.SemaphoreType.DMA
    sems = [dma((16, PIECES))] * 4 + [dma((16, 1))] * 8 + [dma((2 + PIECES,))] * 4 + [dma((8,))] * 4 + [dma((16,))] * 2
    return pl.pallas_call(
        gather_kernel,
        name="gather",
        out_shape=jax.ShapeDtypeStruct((size, size), F32),
        in_specs=[vmem] * 4,
        out_specs=vmem,
        scratch_shapes=[pltpu.VMEM((16, width, size), F32)] * 4
        + [
            pltpu.VMEM((size, size), BF16),
            pltpu.VMEM((16, size, 128), F32),
            pltpu.VMEM((16, size, 128), F32),
            pltpu.VMEM((size, 128), F32),
            pltpu.VMEM((size, 128), F32),
            pltpu.VMEM((width, size), F32),
            pltpu.VMEM((size, size), BF16),
            pltpu.VMEM((size, size), BF16),
            pltpu.VMEM((8, 2, width, size), F32),
            pltpu.VMEM((8, width, size), F32),
            pltpu.VMEM((8, width, size), F32),
            pltpu.VMEM((7, width, size), F32),
            pltpu.VMEM((8, 2, width, 128), F32),
            pltpu.VMEM((8, width, 128), F32),
            pltpu.VMEM((8, width, 128), F32),
            pltpu.VMEM((7, width, 128), F32),
            pltpu.VMEM((16, width, 128), F32),
            pltpu.VMEM((width, 128), F32),
        ]
        + sems,
        compiler_params=pltpu.CompilerParams(
            collective_id=0, has_side_effects=True, vmem_limit_bytes=56 * 1024 * 1024
        ),
    )(left_panel.T, right_panel.T, reflectors.T, matrix)


def solution(mesh):
    in_specs = (P("row", "col"), P("row", "col"), P("row", "col"), P("row", "col"))
    out_specs = P("row", "col")
    return jax.shard_map(local, mesh=mesh, in_specs=in_specs, out_specs=out_specs, check_vma=False)
```
